32 devices in a mesh: blk: 8 (over y, x, core), pix: 4 (over z).
Axes of the slice: x: 2, y: 2, z: 4, core: 2. Of those that a mesh axis runs over, the one named last changes fastest.
Arguments:
- particles: bfloat16 [4096, 16384], P('blk', 'pix'), may hold values from -10 to 10, as said below
- ctf: bfloat16 [4096, 16384], P('blk', 'pix'), may hold values from -1 to 1
- noise_var: float32 [16384], P('pix'), may hold values from 0.5 to 4
- projections: bfloat16 [128, 16384], P('blk', 'pix'), may hold values from -3.1 to 3.1
- orient_class: int32 [128], replicated, may hold values from 0 to 4
- class_prior: float32 [5], replicated, may hold values from -2 to 0
- counts: int32 [8], P('blk'), may hold values from 32 to 512, as said below
Outputs:
- class_field: float32 [128, 16384], P('blk', 'pix')
- normalizer: float32 [4096], P('blk')
The draws below stay inside these ranges and needn't reach their ends.
Inputs may be any that keep to these rules, and one draw needn't show every extreme that they name: `particles`: real values of particle images. Live slots of each index of blk are its first counts slots; some index of blk is full in every draw.
All inputs are finite; a program needn't handle non-finite values.
Results may differ from the reference program's by a relative error of at most 0.0066.
Values may be sent and summed in bfloat16 or wider, within the bound.
No kernel may reach another device: no remote copies, remote signals or barrier semaphores. Data moves between devices by JAX's collectives and lax.ppermute only.
A program may use at most 128 MiB of HBM per device.

```python
import math
import jax
import jax.numpy as jnp
from jax import lax

PIX = 16384
CLASSES = 5
PART_DEV = 512
ORIENTS = 128
PARTICLES = 4096


def common_fields(key):
    base = jax.random.fold_in(key, 7)
    key_proj, key_ctf, key_noise = jax.random.split(base, 3)
    projection_draw = 0.04 * jax.random.truncated_normal(key_proj, -10.0, 10.0, (ORIENTS, PIX), jnp.float32)
    ctf_draw = jax.random.uniform(key_ctf, (PARTICLES, PIX), jnp.float32, -1.0, 1.0)
    noise_draw = jax.random.truncated_normal(key_noise, -6.0, 6.0, (PARTICLES, PIX), jnp.float32)
    return (projection_draw, ctf_draw, noise_draw)


def draw_particles(key, part):
    return common_fields(key)[2].astype(jnp.bfloat16)


def draw_ctf(key, part):
    return common_fields(key)[1].astype(jnp.bfloat16)


def draw_projections(key, part):
    return common_fields(key)[0].astype(jnp.bfloat16)


def draw_counts(key, part):
    shards = PARTICLES // PART_DEV
    key_level, key_full = jax.random.split(jax.random.fold_in(key, 11))
    level = jax.random.randint(key_level, (shards,), 0, 65)
    full_shard = jax.random.randint(key_full, (), 0, shards)
    level = jnp.where(jnp.arange(shards, dtype=jnp.int32) == full_shard, 64, level)
    lowest = PART_DEV // 16
    return (lowest + (PART_DEV - lowest) * level * level * level // 262144).astype(jnp.int32)


def place_ends(array, key, least, top_value):
    extent = array.shape
    place = [jax.random.randint(jax.random.fold_in(key, axis), (), 0, extent[axis]) for axis in range(len(extent))]
    array = array.at[tuple(place)].set(least)
    longest = extent.index(max(extent))
    place[longest] = (place[longest] + 1) % extent[longest]
    return array.at[tuple(place)].set(top_value)


def block_scale(key, shape, cuts, low, largest):
    def one(dim, parts):
        heights = jax.random.uniform(jax.random.fold_in(jax.random.fold_in(key, 6), dim), (parts,), jnp.float32, low / len(cuts), largest / len(cuts))
        return jnp.repeat(jnp.exp(heights), shape[dim] // parts).reshape((-1,) + (1,) * (len(shape) - dim - 1))

    gain = one(*cuts[0])
    for cut in cuts[1:]:
        gain = gain * one(*cut)
    return gain


def setup_inputs(seed: int = 0) -> dict:
    key_of = jax.random.split(jax.random.key(seed), 8)
    particles = draw_particles(jax.random.fold_in(key_of[7], 71), 0)
    ctf = draw_ctf(jax.random.fold_in(key_of[7], 71), 0)
    noise_var = jnp.clip(jnp.exp(math.log(4.0) - 2.0794415 * jax.random.uniform(key_of[2], (PIX,), jnp.float32) ** block_scale(key_of[2], (PIX,), ((0, 4),), -0.2, 0.2)), 0.5, 4.0)
    projections = draw_projections(jax.random.fold_in(key_of[7], 71), 0)
    orient_class = place_ends(jax.random.randint(key_of[4], (ORIENTS,), 0, CLASSES), jax.random.fold_in(key_of[4], 1), 0, CLASSES - 1).astype(jnp.int32)
    class_prior = jnp.clip(jax.random.uniform(key_of[5], (CLASSES,), jnp.float32, -2.0, 0.0), -2.0, 0.0)
    counts = draw_counts(jax.random.fold_in(key_of[7], 71), 0)
    return dict(particles=particles, ctf=ctf, noise_var=noise_var, projections=projections, orient_class=orient_class, class_prior=class_prior, counts=counts)


def reference(particles, ctf, noise_var, projections, orient_class, class_prior, counts):
    inverse = 1.0 / noise_var
    ctf_wide = ctf.astype(jnp.float32)
    weighted = (particles.astype(jnp.float32) * ctf_wide * inverse[None, :]).astype(jnp.bfloat16)
    quadratic = (0.5 * ctf_wide * ctf_wide * inverse[None, :]).astype(jnp.bfloat16)
    proj_wide = projections.astype(jnp.float32)
    square = (proj_wide * proj_wide).astype(jnp.bfloat16)
    cross_term = lax.dot_general(weighted, projections, (((1,), (1,)), ((), ())), preferred_element_type=jnp.float32)
    square_term = lax.dot_general(quadratic, square, (((1,), (1,)), ((), ())), preferred_element_type=jnp.float32)
    scores = cross_term - square_term
    member = orient_class[:, None] == jnp.arange(CLASSES, dtype=jnp.int32)[None, :]
    orient_prior = jnp.sum(jnp.where(member, class_prior[None, :], jnp.float32(0.0)), axis=1)
    logits = scores + orient_prior[None, :]
    peak_score = jnp.max(logits, axis=1)
    log_total = peak_score + jnp.log(jnp.sum(jnp.exp(logits - peak_score[:, None]), axis=1))
    slot_index = jnp.arange(PARTICLES, dtype=jnp.int32) % PART_DEV
    shard_index = jnp.arange(PARTICLES, dtype=jnp.int32) // PART_DEV
    live_slot = slot_index < counts[shard_index]
    normalizer = jnp.where(live_slot, log_total, jnp.float32(0.0))
    weights = jnp.where(live_slot[:, None], jnp.exp(logits - log_total[:, None]), jnp.float32(0.0)).astype(jnp.bfloat16)
    class_field = lax.dot_general(weights, weighted, (((0,), (0,)), ((), ())), preferred_element_type=jnp.float32)
    return class_field, normalizer
```

```python
import functools

import jax
import jax.numpy as jnp
from jax import lax
from jax.experimental import pallas as pl
from jax.experimental.pallas import tpu as pltpu
from jax.sharding import PartitionSpec as P

BF16 = jnp.bfloat16
F32 = jnp.float32
MIB = 1 << 20
VMEM = pl.BlockSpec(memory_space=pltpu.VMEM)
SMEM = pl.BlockSpec(memory_space=pltpu.SMEM)
HBM = pl.BlockSpec(memory_space=pl.ANY)


def swap(value, axis, size, k):
    out = lax.ppermute(value, axis, [(i, i ^ k) for i in range(size)])
    return pltpu.with_memory_space_constraint(out, pltpu.VMEM)


def params(mib):
    return pltpu.CompilerParams(vmem_limit_bytes=mib * MIB)


def cost(flops, moved):
    return pl.CostEstimate(flops=int(flops), bytes_accessed=int(moved), transcendentals=0)


def prepare_kernel(order, rows, particles, ctf, noise, orient_class, class_prior, weighted, quadratic, prior, p_buf, c_buf, p_sem, c_sem):
    steps = p_buf.shape[0]
    tall = p_buf.shape[1]
    loads = []
    for s in range(steps):
        span = pl.ds(s * tall, tall)
        a = pltpu.make_async_copy(particles.at[span], p_buf.at[s], p_sem.at[s])
        b = pltpu.make_async_copy(ctf.at[span], c_buf.at[s], c_sem.at[s])
        a.start()
        b.start()
        loads.append((a, b))
    orients = prior.shape[0]
    me = lax.axis_index("blk")
    classes = orient_class[...]
    table = jnp.zeros(classes.shape, F32)
    for c in range(class_prior.shape[0]):
        table = table + jnp.where(classes == c, class_prior[c], jnp.float32(0.0))
    column = lax.broadcasted_iota(jnp.int32, (rows, orients), 1)
    row = lax.broadcasted_iota(jnp.int32, (rows, orients), 0)
    for slot, k in enumerate(order):
        hit = column == (me ^ k) * rows + row
        picked = jnp.sum(jnp.where(hit, table, jnp.float32(0.0)), axis=1, keepdims=True)
        prior[slot * rows : (slot + 1) * rows, :] = jnp.broadcast_to(picked, (rows, prior.shape[1]))
    inverse = 1.0 / noise[...]
    for s, (a, b) in enumerate(loads):
        a.wait()
        b.wait()
        wide = c_buf[s].astype(F32)
        span = slice(s * tall, (s + 1) * tall)
        weighted[span, :] = (p_buf[s].astype(F32) * wide * inverse).astype(BF16)
        quadratic[span, :] = (0.5 * wide * wide * inverse).astype(BF16)


def prepare(order, rows, parts, particles, ctf, noise, orient_class, class_prior):
    slots, pixels = particles.shape
    steps = 8 if slots % 128 == 0 else 1
    orients = orient_class.shape[0]
    lanes = slots // parts
    return pl.pallas_call(
        functools.partial(prepare_kernel, order, rows),
        out_shape=(
            pltpu.VMEM((slots, pixels), BF16),
            pltpu.VMEM((slots, pixels), BF16),
            pltpu.VMEM((orients, lanes), F32),
        ),
        in_specs=[HBM, HBM, VMEM, VMEM, SMEM],
        out_specs=(VMEM, VMEM, VMEM),
        scratch_shapes=[
            pltpu.VMEM((steps, slots // steps, pixels), BF16),
            pltpu.VMEM((steps, slots // steps, pixels), BF16),
            pltpu.SemaphoreType.DMA((steps,)),
            pltpu.SemaphoreType.DMA((steps,)),
        ],
        compiler_params=params(14),
        cost_estimate=cost(16 * slots * pixels, 8 * slots * pixels),
        name="prepare",
    )(particles, ctf, noise.reshape(1, -1), orient_class.reshape(1, -1), class_prior)


NT = (((1,), (1,)), ((), ()))


def score_kernel(pieces, parts, *refs):
    proj = refs[:pieces]
    weighted, quadratic = refs[pieces : pieces + 2]
    outs = refs[pieces + 2 : pieces + 2 + parts]
    rows_all, square, total = refs[pieces + 2 + parts :]
    rows = proj[0].shape[0]
    for i, piece in enumerate(proj):
        value = piece[...]
        wide = value.astype(F32)
        rows_all[i * rows : (i + 1) * rows, :] = value
        square[i * rows : (i + 1) * rows, :] = (wide * wide).astype(BF16)
    total[...] = lax.dot_general(rows_all[...], weighted[...], NT, preferred_element_type=F32) - lax.dot_general(
        square[...], quadratic[...], NT, preferred_element_type=F32
    )
    quarter = lax.axis_index("pix")
    lanes = outs[0].shape[1]
    for j, out in enumerate(outs):
        start = pl.multiple_of((quarter ^ j) * lanes, lanes)
        out[...] = total[:, pl.ds(start, lanes)]


def score(parts, proj, weighted, quadratic):
    rows, pixels = proj[0].shape
    orients = rows * len(proj)
    slots = weighted.shape[0]
    return pl.pallas_call(
        functools.partial(score_kernel, len(proj), parts),
        out_shape=tuple(pltpu.VMEM((orients, slots // parts), F32) for _ in range(parts)),
        in_specs=[VMEM] * (len(proj) + 2),
        out_specs=(VMEM,) * parts,
        scratch_shapes=[
            pltpu.VMEM((orients, pixels), BF16),
            pltpu.VMEM((orients, pixels), BF16),
            pltpu.VMEM((orients, slots), F32),
        ],
        compiler_params=params(30),
        cost_estimate=cost(4 * orients * slots * pixels, 4 * slots * pixels),
        name="score",
    )(*proj, weighted, quadratic)


def weigh_kernel(parts, *refs):
    prior, counts = refs[parts : parts + 2]
    out = refs[parts + 2]
    logits = refs[0][...]
    for piece in refs[1:parts]:
        logits = logits + piece[...]
    logits = logits + prior[...]
    orients, lanes = logits.shape
    peak = jnp.max(logits, axis=0, keepdims=True)
    log_total = peak + jnp.log(jnp.sum(jnp.exp(logits - peak), axis=0, keepdims=True))
    slot = lax.axis_index("pix") * lanes + lax.broadcasted_iota(jnp.int32, (1, lanes), 1)
    live = slot < counts[0]
    out[:orients, :] = jnp.where(live, jnp.exp(logits - log_total), jnp.float32(0.0)).astype(BF16)
    norm = jnp.where(live, log_total, jnp.float32(0.0))
    high = norm.astype(BF16).astype(F32)
    rest = norm - high
    middle = rest.astype(BF16).astype(F32)
    low = rest - middle
    line = lax.broadcasted_iota(jnp.int32, (16, lanes), 0)
    tail = jnp.where(line == 0, high, jnp.where(line == 1, middle, jnp.where(line == 2, low, jnp.float32(0.0))))
    out[orients:, :] = tail.astype(BF16)


def weigh(pieces, prior, counts):
    orients, lanes = prior.shape
    return pl.pallas_call(
        functools.partial(weigh_kernel, len(pieces)),
        out_shape=pltpu.VMEM((orients + 16, lanes), BF16),
        in_specs=[VMEM] * (len(pieces) + 1) + [SMEM],
        out_specs=VMEM,
        compiler_params=params(8),
        cost_estimate=cost(40 * orients * lanes, 20 * orients * lanes),
        name="weigh",
    )(*pieces, prior, counts)


def field_kernel(parts, *refs):
    pieces = refs[:parts]
    weighted, kept, sent, norm, lhs = refs[parts:]
    orients, slots = lhs.shape
    lanes = slots // parts
    quarter = lax.axis_index("pix")
    for j, piece in enumerate(pieces):
        place = quarter ^ j
        start = pl.multiple_of(place * lanes, lanes)
        lhs[:, pl.ds(start, lanes)] = piece[:orients, :]
        tail = piece[orients:, :].astype(F32)
        norm[pl.ds(place, 1), :] = (tail[0:1] + tail[1:2]) + tail[2:3]
    half = orients // 2
    pixels = weighted.shape[1]
    wide = 1024 if pixels % 1024 == 0 else pixels
    for c in range(pixels // wide):
        span = slice(c * wide, (c + 1) * wide)
        value = jnp.dot(lhs[...], weighted[:, span], preferred_element_type=F32)
        kept[:, span] = value[:half]
        sent[:, span] = value[half:].astype(BF16)


def field(pieces, weighted):
    slots, pixels = weighted.shape
    parts = len(pieces)
    orients = pieces[0].shape[0] - 16
    return pl.pallas_call(
        functools.partial(field_kernel, parts),
        out_shape=(
            pltpu.VMEM((orients // 2, pixels), F32),
            pltpu.VMEM((orients // 2, pixels), BF16),
            jax.ShapeDtypeStruct((parts, slots // parts), F32),
        ),
        in_specs=[VMEM] * (parts + 1),
        out_specs=(VMEM, VMEM, VMEM),
        scratch_shapes=[pltpu.VMEM((orients, slots), BF16)],
        compiler_params=params(16),
        cost_estimate=cost(2 * orients * slots * pixels, 2 * slots * pixels),
        name="field",
    )(*pieces, weighted)


def pair_kernel(kept, got, own, *outs):
    rows = own.shape[0]
    own[...] = kept[:rows, :] + got[:rows, :].astype(F32)
    for i, out in enumerate(outs):
        span = slice((i + 1) * rows, (i + 2) * rows)
        out[...] = (kept[span, :] + got[span, :].astype(F32)).astype(BF16)


def pair(kept, got, rows):
    orients, pixels = kept.shape
    return pl.pallas_call(
        pair_kernel,
        out_shape=(pltpu.VMEM((rows, pixels), F32),) + tuple(pltpu.VMEM((rows, pixels), BF16) for _ in range(orients // rows - 1)),
        in_specs=[VMEM, VMEM],
        out_specs=(VMEM,) * (orients // rows),
        compiler_params=params(8),
        cost_estimate=cost(2 * orients * pixels, 8 * orients * pixels),
        name="pair",
    )(kept, got)


def final_kernel(own, *refs):
    total = own[...]
    for piece in refs[:-1]:
        total = total + piece[...].astype(F32)
    refs[-1][...] = total


def final(own, pieces):
    return pl.pallas_call(
        final_kernel,
        out_shape=jax.ShapeDtypeStruct(own.shape, F32),
        in_specs=[VMEM] * (len(pieces) + 1),
        out_specs=VMEM,
        compiler_params=params(16),
        cost_estimate=cost(own.size * len(pieces), 4 * own.size * len(pieces)),
        name="final",
    )(own, *pieces)


def body(blk, pix, particles, ctf, noise_var, projections, orient_class, class_prior, counts):
    rows = projections.shape[0]
    even = list(range(2, blk, 2))
    order = [0] + even + [k ^ 1 for k in [0] + even]
    far = {k: swap(projections, "blk", blk, k) for k in reversed(even)}
    near = swap(projections, "blk", blk, 1)
    weighted, quadratic, prior = prepare(order, rows, pix, particles, ctf, noise_var, orient_class, class_prior)
    proj = [projections] + [far[k] for k in even] + [near] + [swap(far[k], "blk", blk, 1) for k in even]
    chunks = score(pix, proj, weighted, quadratic)
    pieces = [chunks[0]] + [swap(chunks[j], "pix", pix, j) for j in range(1, pix)]
    weights = weigh(pieces, prior, counts)
    parts = [weights] + [swap(weights, "pix", pix, j) for j in range(1, pix)]
    kept, sent, norm = field(parts, weighted)
    own, *out = pair(kept, swap(sent, "blk", blk, 1), rows)
    got = [swap(piece, "blk", blk, k) for piece, k in zip(out, even)]
    return final(own, got), norm.reshape(-1)


def solution(mesh):
    placed = (P("blk", "pix"), P("blk", "pix"), P("pix"), P("blk", "pix"), P(), P(), P("blk"))
    return jax.shard_map(
        functools.partial(body, mesh.shape["blk"], mesh.shape["pix"]),
        mesh=mesh,
        in_specs=placed,
        out_specs=(P("blk", "pix"), P("blk")),
        check_vma=False,
    )
```

```python
import functools

import jax
import jax.numpy as jnp
from jax import lax
from jax.experimental import pallas as pl
from jax.experimental.pallas import tpu as pltpu
from jax.sharding import PartitionSpec as P


BF16 = jnp.bfloat16
F32 = jnp.float32
MIB = 1 << 20
VMEM = pl.BlockSpec(memory_space=pltpu.VMEM)
SMEM = pl.BlockSpec(memory_space=pltpu.SMEM)
HBM = pl.BlockSpec(memory_space=pltpu.HBM)


def swap(value, axis, size, k):
    out = lax.ppermute(value, axis, [(i, i ^ k) for i in range(size)])
    return pltpu.with_memory_space_constraint(out, pltpu.VMEM)


def params(mib):
    return pltpu.CompilerParams(vmem_limit_bytes=mib * MIB)


def cost(flops, moved):
    return pl.CostEstimate(flops=int(flops), bytes_accessed=int(moved), transcendentals=0)


def prepare_kernel(order, rows, particles, ctf, noise, orient_class, class_prior, weighted, quadratic, prior, *scratch):
    p_buf, c_buf, n_buf, o_buf, r_buf, p_sem, c_sem, small_sem = scratch
    steps = p_buf.shape[0]
    tall = p_buf.shape[1]
    loads = []
    small = []
    for i, (source, target) in enumerate(((noise, n_buf), (orient_class, o_buf), (class_prior, r_buf))):
        small.append(pltpu.make_async_copy(source, target, small_sem.at[i]))
        small[-1].start()
    for s in range(steps):
        span = pl.ds(s * tall, tall)
        a = pltpu.make_async_copy(particles.at[span], p_buf.at[s], p_sem.at[s])
        b = pltpu.make_async_copy(ctf.at[span], c_buf.at[s], c_sem.at[s])
        a.start()
        b.start()
        loads.append((a, b))
    orients = prior.shape[0]
    me = lax.axis_index("blk")
    for copy in small:
        copy.wait()
    classes = o_buf[...]
    table = jnp.zeros(classes.shape, F32)
    for c in range(r_buf.shape[1]):
        table = table + jnp.where(classes == c, r_buf[0:1, c : c + 1], jnp.float32(0.0))
    column = lax.broadcasted_iota(jnp.int32, (rows, orients), 1)
    row = lax.broadcasted_iota(jnp.int32, (rows, orients), 0)
    for slot, k in enumerate(order):
        hit = column == (me ^ k) * rows + row
        picked = jnp.sum(jnp.where(hit, table, jnp.float32(0.0)), axis=1, keepdims=True)
        prior[slot * rows : (slot + 1) * rows, :] = jnp.broadcast_to(picked, (rows, prior.shape[1]))
    inverse = 1.0 / n_buf[...]
    for s, (a, b) in enumerate(loads):
        a.wait()
        b.wait()
        wide = c_buf[s].astype(F32)
        scaled = wide * inverse
        span = slice(s * tall, (s + 1) * tall)
        weighted[span, :] = (p_buf[s].astype(F32) * scaled).astype(BF16)
        quadratic[span, :] = (wide * scaled).astype(BF16)


def prepare(order, rows, parts, particles, ctf, noise, orient_class, class_prior):
    slots, pixels = particles.shape
    steps = 8 if slots % 128 == 0 else 1
    orients = orient_class.shape[0]
    lanes = slots // parts
    operands = (particles, ctf, noise.reshape(1, -1), orient_class.reshape(1, -1), class_prior.reshape(1, -1))
    return pl.pallas_call(
        functools.partial(prepare_kernel, order, rows),
        out_shape=(
            pltpu.VMEM((slots, pixels), BF16),
            pltpu.VMEM((slots, pixels), BF16),
            pltpu.VMEM((orients, lanes), F32),
        ),
        in_specs=[HBM] * 5,
        out_specs=(VMEM, VMEM, VMEM),
        scratch_shapes=[
            pltpu.VMEM((steps, slots // steps, pixels), BF16),
            pltpu.VMEM((steps, slots // steps, pixels), BF16),
            pltpu.VMEM((1, pixels), F32),
            pltpu.VMEM((1, orients), jnp.int32),
            pltpu.VMEM((1, class_prior.shape[0]), F32),
            pltpu.SemaphoreType.DMA((steps,)),
            pltpu.SemaphoreType.DMA((steps,)),
            pltpu.SemaphoreType.DMA((3,)),
        ],
        compiler_params=params(14),
        cost_estimate=cost(16 * slots * pixels, 8 * slots * pixels),
        name="prepare",
    )(*(pltpu.with_memory_space_constraint(value, pltpu.HBM) for value in operands))


NT = (((1,), (1,)), ((), ()))


def score_kernel(pieces, parts, *refs):
    proj = refs[:pieces]
    weighted, quadratic = refs[pieces : pieces + 2]
    outs = refs[pieces + 2 : pieces + 2 + parts]
    rows_all, square, total = refs[pieces + 2 + parts :]
    rows = proj[0].shape[0]
    for i, piece in enumerate(proj):
        value = piece[...]
        wide = value.astype(F32)
        rows_all[i * rows : (i + 1) * rows, :] = value
        square[i * rows : (i + 1) * rows, :] = (0.5 * wide * wide).astype(BF16)
    total[...] = lax.dot_general(rows_all[...], weighted[...], NT, preferred_element_type=F32) - lax.dot_general(
        square[...], quadratic[...], NT, preferred_element_type=F32
    )
    quarter = lax.axis_index("pix")
    lanes = outs[0].shape[1]
    for j, out in enumerate(outs):
        start = pl.multiple_of((quarter ^ j) * lanes, lanes)
        out[...] = total[:, pl.ds(start, lanes)]


def score(parts, proj, weighted, quadratic):
    rows, pixels = proj[0].shape
    orients = rows * len(proj)
    slots = weighted.shape[0]
    return pl.pallas_call(
        functools.partial(score_kernel, len(proj), parts),
        out_shape=tuple(pltpu.VMEM((orients, slots // parts), F32) for _ in range(parts)),
        in_specs=[VMEM] * (len(proj) + 2),
        out_specs=(VMEM,) * parts,
        scratch_shapes=[
            pltpu.VMEM((orients, pixels), BF16),
            pltpu.VMEM((orients, pixels), BF16),
            pltpu.VMEM((orients, slots), F32),
        ],
        compiler_params=params(30),
        cost_estimate=cost(4 * orients * slots * pixels, 4 * slots * pixels),
        name="score",
    )(*proj, weighted, quadratic)


def weigh_kernel(parts, *refs):
    prior, counts = refs[parts : parts + 2]
    out = refs[parts + 2]
    logits = refs[0][...]
    for piece in refs[1:parts]:
        logits = logits + piece[...]
    logits = logits + prior[...]
    orients, lanes = logits.shape
    peak = jnp.max(logits, axis=0, keepdims=True)
    log_total = peak + jnp.log(jnp.sum(jnp.exp(logits - peak), axis=0, keepdims=True))
    slot = lax.axis_index("pix") * lanes + lax.broadcasted_iota(jnp.int32, (1, lanes), 1)
    live = slot < counts[0]
    out[:orients, :] = jnp.where(live, jnp.exp(logits - log_total), jnp.float32(0.0)).astype(BF16)
    norm = jnp.where(live, log_total, jnp.float32(0.0))
    high = norm.astype(BF16).astype(F32)
    rest = norm - high
    middle = rest.astype(BF16).astype(F32)
    low = rest - middle
    line = lax.broadcasted_iota(jnp.int32, (16, lanes), 0)
    tail = jnp.where(line == 0, high, jnp.where(line == 1, middle, jnp.where(line == 2, low, jnp.float32(0.0))))
    out[orients:, :] = tail.astype(BF16)


def weigh(pieces, prior, counts):
    orients, lanes = prior.shape
    return pl.pallas_call(
        functools.partial(weigh_kernel, len(pieces)),
        out_shape=pltpu.VMEM((orients + 16, lanes), BF16),
        in_specs=[VMEM] * (len(pieces) + 1) + [SMEM],
        out_specs=VMEM,
        compiler_params=params(8),
        cost_estimate=cost(40 * orients * lanes, 20 * orients * lanes),
        name="weigh",
    )(*pieces, prior, counts)


def field_kernel(parts, *refs):
    pieces = refs[:parts]
    weighted, kept, sent, norm, lhs = refs[parts:]
    orients, slots = lhs.shape
    lanes = slots // parts
    quarter = lax.axis_index("pix")
    for j, piece in enumerate(pieces):
        place = quarter ^ j
        start = pl.multiple_of(place * lanes, lanes)
        lhs[:, pl.ds(start, lanes)] = piece[:orients, :]
        tail = piece[orients:, :].astype(F32)
        norm[pl.ds(place, 1), :] = (tail[0:1] + tail[1:2]) + tail[2:3]
    half = orients // 2
    pixels = weighted.shape[1]
    wide = 1024 if pixels % 1024 == 0 else pixels
    for c in range(pixels // wide):
        span = slice(c * wide, (c + 1) * wide)
        value = jnp.dot(lhs[...], weighted[:, span], preferred_element_type=F32)
        kept[:, span] = value[:half]
        sent[:, span] = value[half:].astype(BF16)


def field(pieces, weighted):
    slots, pixels = weighted.shape
    parts = len(pieces)
    orients = pieces[0].shape[0] - 16
    return pl.pallas_call(
        functools.partial(field_kernel, parts),
        out_shape=(
            pltpu.VMEM((orients // 2, pixels), F32),
            pltpu.VMEM((orients // 2, pixels), BF16),
            jax.ShapeDtypeStruct((parts, slots // parts), F32),
        ),
        in_specs=[VMEM] * (parts + 1),
        out_specs=(VMEM, VMEM, VMEM),
        scratch_shapes=[pltpu.VMEM((orients, slots), BF16)],
        compiler_params=params(16),
        cost_estimate=cost(2 * orients * slots * pixels, 2 * slots * pixels),
        name="field",
    )(*pieces, weighted)


def pair_kernel(kept, got, own, *outs):
    rows = own.shape[0]
    own[...] = kept[:rows, :] + got[:rows, :].astype(F32)
    for i, out in enumerate(outs):
        span = slice((i + 1) * rows, (i + 2) * rows)
        out[...] = (kept[span, :] + got[span, :].astype(F32)).astype(BF16)


def pair(kept, got, rows):
    orients, pixels = kept.shape
    return pl.pallas_call(
        pair_kernel,
        out_shape=(pltpu.VMEM((rows, pixels), F32),) + tuple(pltpu.VMEM((rows, pixels), BF16) for _ in range(orients // rows - 1)),
        in_specs=[VMEM, VMEM],
        out_specs=(VMEM,) * (orients // rows),
        compiler_params=params(8),
        cost_estimate=cost(2 * orients * pixels, 8 * orients * pixels),
        name="pair",
    )(kept, got)


def final_kernel(own, *refs):
    total = own[...]
    for piece in refs[:-1]:
        total = total + piece[...].astype(F32)
    refs[-1][...] = total


def final(own, pieces):
    return pl.pallas_call(
        final_kernel,
        out_shape=jax.ShapeDtypeStruct(own.shape, F32),
        in_specs=[VMEM] * (len(pieces) + 1),
        out_specs=VMEM,
        compiler_params=params(16),
        cost_estimate=cost(own.size * len(pieces), 4 * own.size * len(pieces)),
        name="final",
    )(own, *pieces)


def body(blk, pix, particles, ctf, noise_var, projections, orient_class, class_prior, counts):
    rows = projections.shape[0]
    even = list(range(2, blk, 2))
    order = [0] + even + [k ^ 1 for k in [0] + even]
    far = {}
    for k in reversed(even):
        far[k] = swap(projections, "blk", blk, k)
    near = swap(projections, "blk", blk, 1)
    weighted, quadratic, prior = prepare(order, rows, pix, particles, ctf, noise_var, orient_class, class_prior)
    proj = [projections] + [far[k] for k in even] + [near] + [swap(far[k], "blk", blk, 1) for k in even]
    chunks = score(pix, proj, weighted, quadratic)
    pieces = [chunks[0]] + [swap(chunks[j], "pix", pix, j) for j in range(1, pix)]
    weights = weigh(pieces, prior, counts)
    parts = [weights] + [swap(weights, "pix", pix, j) for j in range(1, pix)]
    kept, sent, norm = field(parts, weighted)
    own, *out = pair(kept, swap(sent, "blk", blk, 1), rows)
    got = [swap(piece, "blk", blk, k) for piece, k in zip(out, even)]
    return final(own, got), norm.reshape(-1)


def solution(mesh):
    placed = (P("blk", "pix"), P("blk", "pix"), P("pix"), P("blk", "pix"), P(), P(), P("blk"))
    return jax.shard_map(
        functools.partial(body, mesh.shape["blk"], mesh.shape["pix"]),
        mesh=mesh,
        in_specs=placed,
        out_specs=(P("blk", "pix"), P("blk")),
        check_vma=False,
    )
```

```python
import functools

import jax
import jax.numpy as jnp
from jax import lax
from jax.experimental import pallas as pl
from jax.experimental.pallas import tpu as pltpu
from jax.sharding import PartitionSpec as P


BF16 = jnp.bfloat16
F32 = jnp.float32
MIB = 1 << 20
VMEM = pl.BlockSpec(memory_space=pltpu.VMEM)
SMEM = pl.BlockSpec(memory_space=pltpu.SMEM)
HBM = pl.BlockSpec(memory_space=pltpu.HBM)


def swap(value, axis, size, k):
    out = lax.ppermute(value, axis, [(i, i ^ k) for i in range(size)])
    return pltpu.with_memory_space_constraint(out, pltpu.VMEM)


def params(mib):
    return pltpu.CompilerParams(vmem_limit_bytes=mib * MIB)


def cost(flops, moved):
    return pl.CostEstimate(flops=int(flops), bytes_accessed=int(moved), transcendentals=0)


def prepare_kernel(order, rows, particles, ctf, noise, orient_class, class_prior, weighted, quadratic, prior, *scratch):
    p_buf, c_buf, n_buf, o_buf, r_buf, p_sem, c_sem, small_sem = scratch
    steps, tall, _ = p_buf.shape
    small = []
    for i, (source, target) in enumerate(((noise, n_buf), (orient_class, o_buf), (class_prior, r_buf))):
        small.append(pltpu.make_async_copy(source, target, small_sem.at[i]))
        small[-1].start()
    loads = []
    for s in range(steps):
        span = pl.ds(s * tall, tall)
        a = pltpu.make_async_copy(particles.at[span], p_buf.at[s], p_sem.at[s])
        b = pltpu.make_async_copy(ctf.at[span], c_buf.at[s], c_sem.at[s])
        loads.append((a, b))
    ahead = min(4, steps)
    for a, b in loads[:ahead]:
        a.start()
        b.start()
    for copy in small:
        copy.wait()
    inverse = 1.0 / n_buf[...]
    orients = prior.shape[0]
    me = lax.axis_index("blk")
    classes = o_buf[...]
    table = jnp.zeros(classes.shape, F32)
    for c in range(r_buf.shape[1]):
        table = table + jnp.where(classes == c, r_buf[0:1, c : c + 1], jnp.float32(0.0))
    column = lax.broadcasted_iota(jnp.int32, (rows, orients), 1)
    row = lax.broadcasted_iota(jnp.int32, (rows, orients), 0)
    for slot, k in enumerate(order):
        hit = column == (me ^ k) * rows + row
        picked = jnp.sum(jnp.where(hit, table, jnp.float32(0.0)), axis=1, keepdims=True)
        prior[slot * rows : (slot + 1) * rows, :] = jnp.broadcast_to(picked, (rows, prior.shape[1]))
    for s, (a, b) in enumerate(loads):
        a.wait()
        b.wait()
        if s + ahead < steps:
            for copy in loads[s + ahead]:
                copy.start()
        span = slice(s * tall, (s + 1) * tall)
        wide = c_buf[s].astype(F32)
        scaled = wide * inverse
        weighted[span, :] = (p_buf[s].astype(F32) * scaled).astype(BF16)
        quadratic[span, :] = (wide * scaled).astype(BF16)


def prepare(order, rows, parts, particles, ctf, noise, orient_class, class_prior):
    slots, pixels = particles.shape
    steps = 8 if slots % 128 == 0 else 1
    orients = orient_class.shape[1]
    operands = (particles, ctf, noise, orient_class, class_prior)
    return pl.pallas_call(
        functools.partial(prepare_kernel, order, rows),
        out_shape=(
            pltpu.VMEM((slots, pixels), BF16),
            pltpu.VMEM((slots, pixels), BF16),
            pltpu.VMEM((orients, slots // parts), F32),
        ),
        in_specs=[HBM] * 5,
        out_specs=(VMEM, VMEM, VMEM),
        scratch_shapes=[
            pltpu.VMEM((steps, slots // steps, pixels), BF16),
            pltpu.VMEM((steps, slots // steps, pixels), BF16),
            pltpu.VMEM((1, pixels), F32),
            pltpu.VMEM((1, orients), jnp.int32),
            pltpu.VMEM((1, class_prior.shape[1]), F32),
            pltpu.SemaphoreType.DMA((steps,)),
            pltpu.SemaphoreType.DMA((steps,)),
            pltpu.SemaphoreType.DMA((3,)),
        ],
        compiler_params=params(14),
        cost_estimate=cost(16 * slots * pixels, 8 * slots * pixels),
        name="prepare",
    )(*(pltpu.with_memory_space_constraint(value, pltpu.HBM) for value in operands))


def square_kernel(*refs):
    lines, square = refs[-2:]
    rows = refs[0].shape[0]
    for i, piece in enumerate(refs[:-2]):
        value = piece[...]
        wide = value.astype(F32)
        lines[i * rows : (i + 1) * rows, :] = value
        square[i * rows : (i + 1) * rows, :] = (-0.5 * wide * wide).astype(BF16)


def squares(proj):
    rows, pixels = proj[0].shape
    out = pltpu.VMEM((rows * len(proj), pixels), BF16)
    return pl.pallas_call(
        square_kernel,
        out_shape=(out, out),
        in_specs=[VMEM] * len(proj),
        out_specs=(VMEM, VMEM),
        compiler_params=params(4),
        cost_estimate=cost(1000 * rows * len(proj) * pixels, 6 * rows * len(proj) * pixels),
        name="squares",
    )(*proj)


NT = (((1,), (1,)), ((), ()))


def score_kernel(pieces, parts, *refs):
    proj = refs[:pieces]
    lines, square, weighted, quadratic = refs[pieces : pieces + 4]
    outs = refs[pieces + 4 : pieces + 4 + parts]
    lines_all, square_all, total = refs[pieces + 4 + parts :]
    rows = proj[0].shape[0]
    first = lines.shape[0]
    lines_all[:first, :] = lines[...]
    square_all[:first, :] = square[...]
    for i, piece in enumerate(proj):
        value = piece[...]
        wide = value.astype(F32)
        span = slice(first + i * rows, first + (i + 1) * rows)
        lines_all[span, :] = value
        square_all[span, :] = (-0.5 * wide * wide).astype(BF16)
    total[...] = lax.dot_general(weighted[...], lines_all[...], NT, preferred_element_type=F32) + lax.dot_general(
        quadratic[...], square_all[...], NT, preferred_element_type=F32
    )
    quarter = lax.axis_index("pix")
    lanes = outs[0].shape[1]
    for j, out in enumerate(outs):
        start = pl.multiple_of((quarter ^ j) * lanes, lanes)
        out[...] = total[pl.ds(start, lanes), :].T


def score(parts, proj, lines, square, weighted, quadratic):
    rows, pixels = proj[0].shape
    orients = rows * len(proj) + lines.shape[0]
    slots = weighted.shape[0]
    return pl.pallas_call(
        functools.partial(score_kernel, len(proj), parts),
        out_shape=tuple(pltpu.VMEM((orients, slots // parts), F32) for _ in range(parts)),
        in_specs=[VMEM] * (len(proj) + 4),
        out_specs=(VMEM,) * parts,
        scratch_shapes=[
            pltpu.VMEM((orients, pixels), BF16),
            pltpu.VMEM((orients, pixels), BF16),
            pltpu.VMEM((slots, orients), F32),
        ],
        compiler_params=params(28),
        cost_estimate=cost(4 * orients * slots * pixels, 4 * slots * pixels),
        name="score",
    )(*proj, lines, square, weighted, quadratic)


def weigh_kernel(parts, *refs):
    prior, counts = refs[parts : parts + 2]
    out = refs[parts + 2]
    logits = refs[0][...]
    for piece in refs[1:parts]:
        logits = logits + piece[...]
    logits = logits + prior[...]
    orients, lanes = logits.shape
    peak = jnp.max(logits, axis=0, keepdims=True)
    log_total = peak + jnp.log(jnp.sum(jnp.exp(logits - peak), axis=0, keepdims=True))
    slot = lax.axis_index("pix") * lanes + lax.broadcasted_iota(jnp.int32, (1, lanes), 1)
    live = slot < counts[0]
    out[:orients, :] = jnp.where(live, jnp.exp(logits - log_total), jnp.float32(0.0)).astype(BF16)
    norm = jnp.where(live, log_total, jnp.float32(0.0))
    high = norm.astype(BF16).astype(F32)
    rest = norm - high
    middle = rest.astype(BF16).astype(F32)
    low = rest - middle
    line = lax.broadcasted_iota(jnp.int32, (16, lanes), 0)
    tail = jnp.where(line == 0, high, jnp.where(line == 1, middle, jnp.where(line == 2, low, jnp.float32(0.0))))
    out[orients:, :] = tail.astype(BF16)


def weigh(pieces, prior, counts):
    orients, lanes = prior.shape
    return pl.pallas_call(
        functools.partial(weigh_kernel, len(pieces)),
        out_shape=pltpu.VMEM((orients + 16, lanes), BF16),
        in_specs=[VMEM] * (len(pieces) + 1) + [SMEM],
        out_specs=VMEM,
        compiler_params=params(8),
        cost_estimate=cost(40 * orients * lanes, 20 * orients * lanes),
        name="weigh",
    )(*pieces, prior, counts)


def field_kernel(parts, *refs):
    pieces = refs[:parts]
    weighted, kept, sent, norm, lhs = refs[parts:]
    orients, slots = lhs.shape
    lanes = slots // parts
    quarter = lax.axis_index("pix")
    for j, piece in enumerate(pieces):
        place = quarter ^ j
        start = pl.multiple_of(place * lanes, lanes)
        lhs[:, pl.ds(start, lanes)] = piece[:orients, :]
        tail = piece[orients:, :].astype(F32)
        norm[pl.ds(place, 1), :] = (tail[0:1] + tail[1:2]) + tail[2:3]
    half = orients // 2
    pixels = weighted.shape[1]
    wide = 1024 if pixels % 1024 == 0 else pixels
    for c in range(pixels // wide):
        span = slice(c * wide, (c + 1) * wide)
        value = jnp.dot(lhs[...], weighted[:, span], preferred_element_type=F32)
        kept[:, span] = value[:half]
        sent[:, span] = value[half:].astype(BF16)


def field(pieces, weighted):
    slots, pixels = weighted.shape
    parts = len(pieces)
    orients = pieces[0].shape[0] - 16
    return pl.pallas_call(
        functools.partial(field_kernel, parts),
        out_shape=(
            pltpu.VMEM((orients // 2, pixels), F32),
            pltpu.VMEM((orients // 2, pixels), BF16),
            pltpu.VMEM((parts, slots // parts), F32),
        ),
        in_specs=[VMEM] * (parts + 1),
        out_specs=(VMEM, VMEM, VMEM),
        scratch_shapes=[pltpu.VMEM((orients, slots), BF16)],
        compiler_params=params(16),
        cost_estimate=cost(2 * orients * slots * pixels, 2 * slots * pixels),
        name="field",
    )(*pieces, weighted)


def pair_kernel(kept, got, own, *outs):
    rows = own.shape[0]
    own[...] = kept[:rows, :] + got[:rows, :].astype(F32)
    for i, out in enumerate(outs):
        span = slice((i + 1) * rows, (i + 2) * rows)
        out[...] = (kept[span, :] + got[span, :].astype(F32)).astype(BF16)


def pair(kept, got, rows):
    orients, pixels = kept.shape
    return pl.pallas_call(
        pair_kernel,
        out_shape=(pltpu.VMEM((rows, pixels), F32),) + tuple(pltpu.VMEM((rows, pixels), BF16) for _ in range(orients // rows - 1)),
        in_specs=[VMEM, VMEM],
        out_specs=(VMEM,) * (orients // rows),
        compiler_params=params(8),
        cost_estimate=cost(2 * orients * pixels, 8 * orients * pixels),
        name="pair",
    )(kept, got)


def final_kernel(own, *refs):
    total = own[...]
    for piece in refs[:-1]:
        total = total + piece[...].astype(F32)
    refs[-1][...] = total


def final(own, pieces):
    return pl.pallas_call(
        final_kernel,
        out_shape=jax.ShapeDtypeStruct(own.shape, F32),
        in_specs=[VMEM] * (len(pieces) + 1),
        out_specs=VMEM,
        compiler_params=params(16),
        cost_estimate=cost(own.size * len(pieces), 4 * own.size * len(pieces)),
        name="final",
    )(own, *pieces)


def body(blk, pix, particles, ctf, noise_var, projections, orient_class, class_prior, counts):
    rows = projections.shape[0]
    even = list(range(2, blk, 2))
    order = [0] + even + [k ^ 1 for k in [0] + even]
    noise, orient_class, class_prior = (value.reshape(1, -1) for value in (noise_var, orient_class, class_prior))
    far = {}
    for k in even:
        far[k] = swap(projections, "blk", blk, k)
    near = [swap(projections, "blk", blk, 1)]
    weighted, quadratic, prior = prepare(order, rows, pix, particles, ctf, noise, orient_class, class_prior)
    for k in even:
        near.append(swap(far[k], "blk", blk, 1))
    lines, square = squares([projections] + [far[k] for k in even])
    chunks = score(pix, near, lines, square, weighted, quadratic)
    pieces = [chunks[0]]
    for j in range(1, pix):
        pieces.append(swap(chunks[j], "pix", pix, j))
    weights = weigh(pieces, prior, counts)
    parts = [weights]
    for j in range(1, pix):
        parts.append(swap(weights, "pix", pix, j))
    kept, sent, norm = field(parts, weighted)
    own, *out = pair(kept, swap(sent, "blk", blk, 1), rows)
    got = []
    for piece, k in zip(out, even):
        got.append(swap(piece, "blk", blk, k))
    return final(own, got), norm.reshape(-1)


def solution(mesh):
    placed = (P("blk", "pix"), P("blk", "pix"), P("pix"), P("blk", "pix"), P(), P(), P("blk"))
    return jax.shard_map(
        functools.partial(body, mesh.shape["blk"], mesh.shape["pix"]),
        mesh=mesh,
        in_specs=placed,
        out_specs=(P("blk", "pix"), P("blk")),
        check_vma=False,
    )
```

```python
import functools

import jax
import jax.numpy as jnp
from jax import lax
from jax.experimental import pallas as pl
from jax.experimental.pallas import tpu as pltpu
from jax.sharding import PartitionSpec as P


BF16 = jnp.bfloat16
F32 = jnp.float32
MIB = 1 << 20
VMEM = pl.BlockSpec(memory_space=pltpu.VMEM)
SMEM = pl.BlockSpec(memory_space=pltpu.SMEM)
HBM = pl.BlockSpec(memory_space=pltpu.HBM)


def swap(value, axis, size, k):
    out = lax.ppermute(value, axis, [(i, i ^ k) for i in range(size)])
    return pltpu.with_memory_space_constraint(out, pltpu.VMEM)


def params(mib):
    return pltpu.CompilerParams(vmem_limit_bytes=mib * MIB)


def cost(flops, moved):
    return pl.CostEstimate(flops=int(flops), bytes_accessed=int(moved), transcendentals=0)


def prepare_kernel(order, rows, particles, ctf, noise, orient_class, class_prior, weighted, quadratic, prior, *scratch):
    p_buf, c_buf, n_buf, o_buf, r_buf, p_sem, c_sem, small_sem = scratch
    steps, tall, _ = p_buf.shape
    small = []
    for i, (source, target) in enumerate(((noise, n_buf), (orient_class, o_buf), (class_prior, r_buf))):
        small.append(pltpu.make_async_copy(source, target, small_sem.at[i]))
        small[-1].start()
    loads = []
    for s in range(steps):
        span = pl.ds(s * tall, tall)
        a = pltpu.make_async_copy(particles.at[span], p_buf.at[s], p_sem.at[s])
        b = pltpu.make_async_copy(ctf.at[span], c_buf.at[s], c_sem.at[s])
        loads.append((a, b))
    ahead = min(4, steps)
    for a, b in loads[:ahead]:
        a.start()
        b.start()
    for copy in small:
        copy.wait()
    inverse = 1.0 / n_buf[...]
    orients = prior.shape[0]
    me = lax.axis_index("blk")
    classes = o_buf[...]
    table = jnp.zeros(classes.shape, F32)
    for c in range(r_buf.shape[1]):
        table = table + jnp.where(classes == c, r_buf[0:1, c : c + 1], jnp.float32(0.0))
    column = lax.broadcasted_iota(jnp.int32, (rows, orients), 1)
    row = lax.broadcasted_iota(jnp.int32, (rows, orients), 0)
    for slot, k in enumerate(order):
        hit = column == (me ^ k) * rows + row
        picked = jnp.sum(jnp.where(hit, table, jnp.float32(0.0)), axis=1, keepdims=True)
        prior[slot * rows : (slot + 1) * rows, :] = jnp.broadcast_to(picked, (rows, prior.shape[1]))
    for s, (a, b) in enumerate(loads):
        a.wait()
        b.wait()
        if s + ahead < steps:
            for copy in loads[s + ahead]:
                copy.start()
        span = slice(s * tall, (s + 1) * tall)
        wide = c_buf[s].astype(F32)
        scaled = wide * inverse
        weighted[span, :] = (p_buf[s].astype(F32) * scaled).astype(BF16)
        quadratic[span, :] = (wide * scaled).astype(BF16)


def prepare(order, rows, parts, particles, ctf, noise, orient_class, class_prior):
    slots, pixels = particles.shape
    steps = 8 if slots % 128 == 0 else 1
    orients = orient_class.shape[1]
    operands = (particles, ctf, noise, orient_class, class_prior)
    return pl.pallas_call(
        functools.partial(prepare_kernel, order, rows),
        out_shape=(
            pltpu.VMEM((slots, pixels), BF16),
            pltpu.VMEM((slots, pixels), BF16),
            pltpu.VMEM((orients, slots // parts), F32),
        ),
        in_specs=[HBM] * 5,
        out_specs=(VMEM, VMEM, VMEM),
        scratch_shapes=[
            pltpu.VMEM((steps, slots // steps, pixels), BF16),
            pltpu.VMEM((steps, slots // steps, pixels), BF16),
            pltpu.VMEM((1, pixels), F32),
            pltpu.VMEM((1, orients), jnp.int32),
            pltpu.VMEM((1, class_prior.shape[1]), F32),
            pltpu.SemaphoreType.DMA((steps,)),
            pltpu.SemaphoreType.DMA((steps,)),
            pltpu.SemaphoreType.DMA((3,)),
        ],
        compiler_params=params(14),
        cost_estimate=cost(16 * slots * pixels, 8 * slots * pixels),
        name="prepare",
    )(*(pltpu.with_memory_space_constraint(value, pltpu.HBM) for value in operands))


def square_kernel(*refs):
    lines, square = refs[-2:]
    rows = refs[0].shape[0]
    for i, piece in enumerate(refs[:-2]):
        value = piece[...]
        wide = value.astype(F32)
        lines[i * rows : (i + 1) * rows, :] = value
        square[i * rows : (i + 1) * rows, :] = (-0.5 * wide * wide).astype(BF16)


def squares(proj):
    rows, pixels = proj[0].shape
    out = pltpu.VMEM((rows * len(proj), pixels), BF16)
    return pl.pallas_call(
        square_kernel,
        out_shape=(out, out),
        in_specs=[VMEM] * len(proj),
        out_specs=(VMEM, VMEM),
        compiler_params=params(4),
        cost_estimate=cost(1000 * rows * len(proj) * pixels, 6 * rows * len(proj) * pixels),
        name="squares",
    )(*proj)


NT = (((1,), (1,)), ((), ()))


def score_kernel(pieces, parts, *refs):
    proj = refs[:pieces]
    lines, square, weighted, quadratic = refs[pieces : pieces + 4]
    outs = refs[pieces + 4 : pieces + 4 + parts]
    lines_all, square_all, total = refs[pieces + 4 + parts :]
    rows = proj[0].shape[0]
    first = lines.shape[0]
    lines_all[:first, :] = lines[...]
    square_all[:first, :] = square[...]
    for i, piece in enumerate(proj):
        value = piece[...]
        wide = value.astype(F32)
        span = slice(first + i * rows, first + (i + 1) * rows)
        lines_all[span, :] = value
        square_all[span, :] = (-0.5 * wide * wide).astype(BF16)
    total[...] = lax.dot_general(weighted[...], lines_all[...], NT, preferred_element_type=F32) + lax.dot_general(
        quadratic[...], square_all[...], NT, preferred_element_type=F32
    )
    quarter = lax.axis_index("pix")
    lanes = outs[0].shape[1]
    for j, out in enumerate(outs):
        start = pl.multiple_of((quarter ^ j) * lanes, lanes)
        out[...] = total[pl.ds(start, lanes), :].T


def score(parts, proj, lines, square, weighted, quadratic):
    rows, pixels = proj[0].shape
    orients = rows * len(proj) + lines.shape[0]
    slots = weighted.shape[0]
    return pl.pallas_call(
        functools.partial(score_kernel, len(proj), parts),
        out_shape=tuple(pltpu.VMEM((orients, slots // parts), F32) for _ in range(parts)),
        in_specs=[VMEM] * (len(proj) + 4),
        out_specs=(VMEM,) * parts,
        scratch_shapes=[
            pltpu.VMEM((orients, pixels), BF16),
            pltpu.VMEM((orients, pixels), BF16),
            pltpu.VMEM((slots, orients), F32),
        ],
        compiler_params=params(28),
        cost_estimate=cost(4 * orients * slots * pixels, 4 * slots * pixels),
        name="score",
    )(*proj, lines, square, weighted, quadratic)


def weigh_kernel(parts, *refs):
    prior, counts = refs[parts : parts + 2]
    out = refs[parts + 2]
    logits = refs[0][...]
    for piece in refs[1:parts]:
        logits = logits + piece[...]
    logits = logits + prior[...]
    orients, lanes = logits.shape
    peak = jnp.max(logits, axis=0, keepdims=True)
    log_total = peak + jnp.log(jnp.sum(jnp.exp(logits - peak), axis=0, keepdims=True))
    slot = lax.axis_index("pix") * lanes + lax.broadcasted_iota(jnp.int32, (1, lanes), 1)
    live = slot < counts[0]
    out[:orients, :] = jnp.where(live, jnp.exp(logits - log_total), jnp.float32(0.0)).astype(BF16)
    norm = jnp.where(live, log_total, jnp.float32(0.0))
    high = norm.astype(BF16).astype(F32)
    rest = norm - high
    middle = rest.astype(BF16).astype(F32)
    low = rest - middle
    line = lax.broadcasted_iota(jnp.int32, (16, lanes), 0)
    tail = jnp.where(line == 0, high, jnp.where(line == 1, middle, jnp.where(line == 2, low, jnp.float32(0.0))))
    out[orients:, :] = tail.astype(BF16)


def weigh(pieces, prior, counts):
    orients, lanes = prior.shape
    return pl.pallas_call(
        functools.partial(weigh_kernel, len(pieces)),
        out_shape=pltpu.VMEM((orients + 16, lanes), BF16),
        in_specs=[VMEM] * (len(pieces) + 1) + [SMEM],
        out_specs=VMEM,
        compiler_params=params(8),
        cost_estimate=cost(40 * orients * lanes, 20 * orients * lanes),
        name="weigh",
    )(*pieces, prior, counts)


def field_kernel(parts, *refs):
    pieces = refs[:parts]
    weighted, kept, sent, late, norm, lhs = refs[parts:]
    orients, slots = lhs.shape
    lanes = slots // parts
    quarter = lax.axis_index("pix")
    for j, piece in enumerate(pieces):
        place = quarter ^ j
        start = pl.multiple_of(place * lanes, lanes)
        lhs[:, pl.ds(start, lanes)] = piece[:orients, :]
        tail = piece[orients:, :].astype(F32)
        norm[pl.ds(place, 1), :] = (tail[0:1] + tail[1:2]) + tail[2:3]
    half = orients // 2
    pixels = weighted.shape[1]
    wide = 1024 if pixels % 1024 == 0 else pixels
    for c in range(pixels // wide):
        span = slice(c * wide, (c + 1) * wide)
        value = jnp.dot(lhs[...], weighted[:, span], preferred_element_type=F32)
        kept[:, span] = value[:half]
        rest = value[half:].astype(BF16)
        sent[:, span] = rest[: sent.shape[0]]
        late[:, span] = rest[sent.shape[0] :]


def field(pieces, weighted, first):
    slots, pixels = weighted.shape
    parts = len(pieces)
    orients = pieces[0].shape[0] - 16
    return pl.pallas_call(
        functools.partial(field_kernel, parts),
        out_shape=(
            pltpu.VMEM((orients // 2, pixels), F32),
            pltpu.VMEM((first, pixels), BF16),
            pltpu.VMEM((orients // 2 - first, pixels), BF16),
            pltpu.VMEM((parts, slots // parts), F32),
        ),
        in_specs=[VMEM] * (parts + 1),
        out_specs=(VMEM,) * 4,
        scratch_shapes=[pltpu.VMEM((orients, slots), BF16)],
        compiler_params=params(16),
        cost_estimate=cost(2 * orients * slots * pixels, 2 * slots * pixels),
        name="field",
    )(*pieces, weighted)


def pair_kernel(base, kept, got, *outs):
    rows = outs[0].shape[0]
    for i, out in enumerate(outs):
        span = slice(i * rows, (i + 1) * rows)
        mine = slice(base + i * rows, base + (i + 1) * rows)
        out[...] = (kept[mine, :] + got[span, :].astype(F32)).astype(out.dtype)


def pair(kept, got, rows, base, types):
    orients, pixels = got.shape
    return pl.pallas_call(
        functools.partial(pair_kernel, base),
        out_shape=tuple(pltpu.VMEM((rows, pixels), kind) for kind in types),
        in_specs=[VMEM, VMEM],
        out_specs=(VMEM,) * len(types),
        compiler_params=params(8),
        cost_estimate=cost(2 * orients * pixels, 8 * orients * pixels),
        name="pair",
    )(kept, got)


def final_kernel(own, *refs):
    total = own[...]
    for piece in refs[:-1]:
        total = total + piece[...].astype(F32)
    refs[-1][...] = total


def final(own, pieces):
    return pl.pallas_call(
        final_kernel,
        out_shape=jax.ShapeDtypeStruct(own.shape, F32),
        in_specs=[VMEM] * (len(pieces) + 1),
        out_specs=VMEM,
        compiler_params=params(16),
        cost_estimate=cost(own.size * len(pieces), 4 * own.size * len(pieces)),
        name="final",
    )(own, *pieces)


def body(blk, pix, particles, ctf, noise_var, projections, orient_class, class_prior, counts):
    rows = projections.shape[0]
    even = list(range(2, blk, 2))
    lead = even[:-1] + [0] + even[-1:]
    order = lead + [k ^ 1 for k in lead]
    noise, orient_class, class_prior = (value.reshape(1, -1) for value in (noise_var, orient_class, class_prior))
    far = {0: projections}
    near = {}
    for k in even:
        far[k] = swap(projections, "blk", blk, k)
    near[0] = swap(projections, "blk", blk, 1)
    weighted, quadratic, prior = prepare(order, rows, pix, particles, ctf, noise, orient_class, class_prior)
    for k in even:
        near[k] = swap(far[k], "blk", blk, 1)
    lines, square = squares([far[k] for k in lead])
    chunks = score(pix, [near[k] for k in lead], lines, square, weighted, quadratic)
    pieces = [chunks[0]]
    for j in range(1, pix):
        pieces.append(swap(chunks[j], "pix", pix, j))
    weights = weigh(pieces, prior, counts)
    parts = [weights]
    for j in range(1, pix):
        parts.append(swap(weights, "pix", pix, j))
    first = rows * (len(lead) - 2)
    kept, sent, late, norm = field(parts, weighted, first)
    sent = swap(sent, "blk", blk, 1)
    late = swap(late, "blk", blk, 1)
    out = list(pair(kept, sent, rows, 0, [BF16] * (len(lead) - 2)))
    own, last = pair(kept, late, rows, first, [F32, BF16])
    got = []
    for piece, k in zip(out + [last], even):
        got.append(swap(piece, "blk", blk, k))
    return final(own, got), norm.reshape(-1)


def solution(mesh):
    placed = (P("blk", "pix"), P("blk", "pix"), P("pix"), P("blk", "pix"), P(), P(), P("blk"))
    return jax.shard_map(
        functools.partial(body, mesh.shape["blk"], mesh.shape["pix"]),
        mesh=mesh,
        in_specs=placed,
        out_specs=(P("blk", "pix"), P("blk")),
        check_vma=False,
    )
```

```python
import functools

import jax
import jax.numpy as jnp
from jax import lax
from jax.experimental import pallas as pl
from jax.experimental.pallas import tpu as pltpu
from jax.sharding import PartitionSpec as P


BF16 = jnp.bfloat16
F32 = jnp.float32
MIB = 1 << 20
VMEM = pl.BlockSpec(memory_space=pltpu.VMEM)
SMEM = pl.BlockSpec(memory_space=pltpu.SMEM)
HBM = pl.BlockSpec(memory_space=pltpu.HBM)


def swap(value, axis, size, k):
    out = lax.ppermute(value, axis, [(i, i ^ k) for i in range(size)])
    return pltpu.with_memory_space_constraint(out, pltpu.VMEM)


def params(mib):
    return pltpu.CompilerParams(vmem_limit_bytes=mib * MIB)


def cost(flops, moved):
    return pl.CostEstimate(flops=int(flops), bytes_accessed=int(moved), transcendentals=0)


def prepare_kernel(order, rows, particles, ctf, noise, orient_class, class_prior, weighted, quadratic, prior, *scratch):
    p_buf, c_buf, n_buf, o_buf, r_buf, p_sem, c_sem, small_sem = scratch
    steps, tall, _ = p_buf.shape
    small = []
    for i, (source, target) in enumerate(((noise, n_buf), (orient_class, o_buf), (class_prior, r_buf))):
        small.append(pltpu.make_async_copy(source, target, small_sem.at[i]))
        small[-1].start()
    loads = []
    quarter = lax.axis_index("pix")
    lanes = prior.shape[1]
    for s in range(steps):
        first = (quarter ^ (s * tall // lanes)) * lanes + s * tall % lanes
        span = pl.ds(pl.multiple_of(first, tall), tall)
        a = pltpu.make_async_copy(particles.at[span], p_buf.at[s], p_sem.at[s])
        b = pltpu.make_async_copy(ctf.at[span], c_buf.at[s], c_sem.at[s])
        loads.append((a, b))
    ahead = min(4, steps)
    for a, b in loads[:ahead]:
        a.start()
        b.start()
    for copy in small:
        copy.wait()
    inverse = 1.0 / n_buf[...]
    orients = prior.shape[0]
    me = lax.axis_index("blk")
    classes = o_buf[...]
    table = jnp.zeros(classes.shape, F32)
    for c in range(r_buf.shape[1]):
        table = table + jnp.where(classes == c, r_buf[0:1, c : c + 1], jnp.float32(0.0))
    column = lax.broadcasted_iota(jnp.int32, (rows, orients), 1)
    row = lax.broadcasted_iota(jnp.int32, (rows, orients), 0)
    for slot, k in enumerate(order):
        hit = column == (me ^ k) * rows + row
        picked = jnp.sum(jnp.where(hit, table, jnp.float32(0.0)), axis=1, keepdims=True)
        prior[slot * rows : (slot + 1) * rows, :] = jnp.broadcast_to(picked, (rows, prior.shape[1]))
    for s, (a, b) in enumerate(loads):
        a.wait()
        b.wait()
        if s + ahead < steps:
            for copy in loads[s + ahead]:
                copy.start()
        span = slice(s * tall, (s + 1) * tall)
        wide = c_buf[s].astype(F32)
        scaled = wide * inverse
        weighted[span, :] = (p_buf[s].astype(F32) * scaled).astype(BF16)
        quadratic[span, :] = (wide * scaled).astype(BF16)


def prepare(order, rows, parts, particles, ctf, noise, orient_class, class_prior):
    slots, pixels = particles.shape
    steps = 2 * parts
    orients = orient_class.shape[1]
    operands = (particles, ctf, noise, orient_class, class_prior)
    return pl.pallas_call(
        functools.partial(prepare_kernel, order, rows),
        out_shape=(
            pltpu.VMEM((slots, pixels), BF16),
            pltpu.VMEM((slots, pixels), BF16),
            pltpu.VMEM((orients, slots // parts), F32),
        ),
        in_specs=[HBM] * 5,
        out_specs=(VMEM, VMEM, VMEM),
        scratch_shapes=[
            pltpu.VMEM((steps, slots // steps, pixels), BF16),
            pltpu.VMEM((steps, slots // steps, pixels), BF16),
            pltpu.VMEM((1, pixels), F32),
            pltpu.VMEM((1, orients), jnp.int32),
            pltpu.VMEM((1, class_prior.shape[1]), F32),
            pltpu.SemaphoreType.DMA((steps,)),
            pltpu.SemaphoreType.DMA((steps,)),
            pltpu.SemaphoreType.DMA((3,)),
        ],
        compiler_params=params(14),
        cost_estimate=cost(16 * slots * pixels, 8 * slots * pixels),
        name="prepare",
    )(*(pltpu.with_memory_space_constraint(value, pltpu.HBM) for value in operands))


def square_kernel(*refs):
    lines, square = refs[-2:]
    rows = refs[0].shape[0]
    for i, piece in enumerate(refs[:-2]):
        value = piece[...]
        wide = value.astype(F32)
        lines[i * rows : (i + 1) * rows, :] = value
        square[i * rows : (i + 1) * rows, :] = (-0.5 * wide * wide).astype(BF16)


def squares(proj):
    rows, pixels = proj[0].shape
    out = pltpu.VMEM((rows * len(proj), pixels), BF16)
    return pl.pallas_call(
        square_kernel,
        out_shape=(out, out),
        in_specs=[VMEM] * len(proj),
        out_specs=(VMEM, VMEM),
        compiler_params=params(4),
        cost_estimate=cost(1000 * rows * len(proj) * pixels, 6 * rows * len(proj) * pixels),
        name="squares",
    )(*proj)


NT = (((1,), (1,)), ((), ()))


def score_kernel(pieces, *refs):
    proj = refs[:pieces]
    lines, square, weighted, quadratic = refs[pieces : pieces + 4]
    *outs, lines_all, square_all = refs[pieces + 4 :]
    rows = proj[0].shape[0]
    first = lines.shape[0]
    lines_all[:first, :] = lines[...]
    square_all[:first, :] = square[...]
    for i, piece in enumerate(proj):
        value = piece[...]
        wide = value.astype(F32)
        span = slice(first + i * rows, first + (i + 1) * rows)
        lines_all[span, :] = value
        square_all[span, :] = (-0.5 * wide * wide).astype(BF16)
    lanes = outs[0].shape[1]
    total = lax.dot_general(weighted[lanes:, :], lines_all[...], NT, preferred_element_type=F32) + lax.dot_general(
        quadratic[lanes:, :], square_all[...], NT, preferred_element_type=F32
    )
    for j, out in enumerate(outs):
        out[...] = total[j * lanes : (j + 1) * lanes, :].T


def score(parts, proj, lines, square, weighted, quadratic):
    rows, pixels = proj[0].shape
    orients = rows * len(proj) + lines.shape[0]
    slots = weighted.shape[0]
    return pl.pallas_call(
        functools.partial(score_kernel, len(proj)),
        out_shape=tuple(pltpu.VMEM((orients, slots // parts), F32) for _ in range(parts - 1))
        + (pltpu.VMEM((orients, pixels), BF16),) * 2,
        in_specs=[VMEM] * (len(proj) + 4),
        out_specs=(VMEM,) * (parts + 1),
        compiler_params=params(12),
        cost_estimate=cost(4 * orients * slots * pixels, 4 * slots * pixels),
        name="score",
    )(*proj, lines, square, weighted, quadratic)


def own_kernel(lines, square, weighted, quadratic, out):
    lanes = out.shape[1]
    total = lax.dot_general(weighted[:lanes, :], lines[...], NT, preferred_element_type=F32) + lax.dot_general(
        quadratic[:lanes, :], square[...], NT, preferred_element_type=F32
    )
    out[...] = total.T


def own_score(parts, lines, square, weighted, quadratic):
    orients, pixels = lines.shape
    lanes = weighted.shape[0] // parts
    return pl.pallas_call(
        own_kernel,
        out_shape=pltpu.VMEM((orients, lanes), F32),
        in_specs=[VMEM] * 4,
        out_specs=VMEM,
        compiler_params=params(12),
        cost_estimate=cost(4 * orients * lanes * pixels, 4 * lanes * pixels),
        name="own_score",
    )(lines, square, weighted, quadratic)


def weigh_kernel(parts, *refs):
    prior, counts = refs[parts : parts + 2]
    out = refs[parts + 2]
    logits = refs[0][...]
    for piece in refs[1:parts]:
        logits = logits + piece[...]
    logits = logits + prior[...]
    orients, lanes = logits.shape
    peak = jnp.max(logits, axis=0, keepdims=True)
    log_total = peak + jnp.log(jnp.sum(jnp.exp(logits - peak), axis=0, keepdims=True))
    slot = lax.axis_index("pix") * lanes + lax.broadcasted_iota(jnp.int32, (1, lanes), 1)
    live = slot < counts[0]
    out[:orients, :] = jnp.where(live, jnp.exp(logits - log_total), jnp.float32(0.0)).astype(BF16)
    norm = jnp.where(live, log_total, jnp.float32(0.0))
    high = norm.astype(BF16).astype(F32)
    rest = norm - high
    middle = rest.astype(BF16).astype(F32)
    low = rest - middle
    line = lax.broadcasted_iota(jnp.int32, (16, lanes), 0)
    tail = jnp.where(line == 0, high, jnp.where(line == 1, middle, jnp.where(line == 2, low, jnp.float32(0.0))))
    out[orients:, :] = tail.astype(BF16)


def weigh(pieces, prior, counts):
    orients, lanes = prior.shape
    return pl.pallas_call(
        functools.partial(weigh_kernel, len(pieces)),
        out_shape=pltpu.VMEM((orients + 16, lanes), BF16),
        in_specs=[VMEM] * (len(pieces) + 1) + [SMEM],
        out_specs=VMEM,
        compiler_params=params(8),
        cost_estimate=cost(40 * orients * lanes, 20 * orients * lanes),
        name="weigh",
    )(*pieces, prior, counts)


def field_kernel(parts, *refs):
    pieces = refs[:parts]
    weighted, kept, sent, late, norm, lhs = refs[parts:]
    orients, slots = lhs.shape
    lanes = slots // parts
    quarter = lax.axis_index("pix")
    for j, piece in enumerate(pieces):
        place = quarter ^ j
        lhs[:, j * lanes : (j + 1) * lanes] = piece[:orients, :]
        tail = piece[orients:, :].astype(F32)
        norm[pl.ds(place, 1), :] = (tail[0:1] + tail[1:2]) + tail[2:3]
    half = orients // 2
    pixels = weighted.shape[1]
    wide = 1024 if pixels % 1024 == 0 else pixels
    for c in range(pixels // wide):
        span = slice(c * wide, (c + 1) * wide)
        value = jnp.dot(lhs[...], weighted[:, span], preferred_element_type=F32)
        kept[:, span] = value[:half]
        rest = value[half:].astype(BF16)
        sent[:, span] = rest[: sent.shape[0]]
        late[:, span] = rest[sent.shape[0] :]


def field(pieces, weighted, first):
    slots, pixels = weighted.shape
    parts = len(pieces)
    orients = pieces[0].shape[0] - 16
    return pl.pallas_call(
        functools.partial(field_kernel, parts),
        out_shape=(
            pltpu.VMEM((orients // 2, pixels), F32),
            pltpu.VMEM((first, pixels), BF16),
            pltpu.VMEM((orients // 2 - first, pixels), BF16),
            pltpu.VMEM((parts, slots // parts), F32),
        ),
        in_specs=[VMEM] * (parts + 1),
        out_specs=(VMEM,) * 4,
        scratch_shapes=[pltpu.VMEM((orients, slots), BF16)],
        compiler_params=params(16),
        cost_estimate=cost(2 * orients * slots * pixels, 2 * slots * pixels),
        name="field",
    )(*pieces, weighted)


def pair_kernel(base, kept, got, *outs):
    rows = outs[0].shape[0]
    for i, out in enumerate(outs):
        span = slice(i * rows, (i + 1) * rows)
        mine = slice(base + i * rows, base + (i + 1) * rows)
        out[...] = (kept[mine, :] + got[span, :].astype(F32)).astype(out.dtype)


def pair(kept, got, rows, base, types):
    orients, pixels = got.shape
    return pl.pallas_call(
        functools.partial(pair_kernel, base),
        out_shape=tuple(pltpu.VMEM((rows, pixels), kind) for kind in types),
        in_specs=[VMEM, VMEM],
        out_specs=(VMEM,) * len(types),
        compiler_params=params(8),
        cost_estimate=cost(2 * orients * pixels, 8 * orients * pixels),
        name="pair",
    )(kept, got)


def final_kernel(own, *refs):
    total = own[...]
    for piece in refs[:-1]:
        total = total + piece[...].astype(F32)
    refs[-1][...] = total


def final(own, pieces):
    return pl.pallas_call(
        final_kernel,
        out_shape=jax.ShapeDtypeStruct(own.shape, F32),
        in_specs=[VMEM] * (len(pieces) + 1),
        out_specs=VMEM,
        compiler_params=params(16),
        cost_estimate=cost(own.size * len(pieces), 4 * own.size * len(pieces)),
        name="final",
    )(own, *pieces)


def body(blk, pix, particles, ctf, noise_var, projections, orient_class, class_prior, counts):
    rows = projections.shape[0]
    even = list(range(2, blk, 2))
    lead = even[:-1] + [0] + even[-1:]
    order = lead + [k ^ 1 for k in lead]
    noise, orient_class, class_prior = (value.reshape(1, -1) for value in (noise_var, orient_class, class_prior))
    far = {0: projections}
    near = {}
    for k in even:
        far[k] = swap(projections, "blk", blk, k)
    near[0] = swap(projections, "blk", blk, 1)
    weighted, quadratic, prior = prepare(order, rows, pix, particles, ctf, noise, orient_class, class_prior)
    for k in even:
        near[k] = swap(far[k], "blk", blk, 1)
    lines, square = squares([far[k] for k in lead])
    *chunks, lines, square = score(pix, [near[k] for k in lead], lines, square, weighted, quadratic)
    pieces = []
    for j in range(1, pix):
        pieces.append(swap(chunks[j - 1], "pix", pix, j))
    pieces.insert(0, own_score(pix, lines, square, weighted, quadratic))
    weights = weigh(pieces, prior, counts)
    parts = [weights]
    for j in range(1, pix):
        parts.append(swap(weights, "pix", pix, j))
    first = rows * (len(lead) - 2)
    kept, sent, late, norm = field(parts, weighted, first)
    sent = swap(sent, "blk", blk, 1)
    late = swap(late, "blk", blk, 1)
    out = list(pair(kept, sent, rows, 0, [BF16] * (len(lead) - 2)))
    own, last = pair(kept, late, rows, first, [F32, BF16])
    got = []
    for piece, k in zip(out + [last], even):
        got.append(swap(piece, "blk", blk, k))
    return final(own, got), norm.reshape(-1)


def solution(mesh):
    placed = (P("blk", "pix"), P("blk", "pix"), P("pix"), P("blk", "pix"), P(), P(), P("blk"))
    return jax.shard_map(
        functools.partial(body, mesh.shape["blk"], mesh.shape["pix"]),
        mesh=mesh,
        in_specs=placed,
        out_specs=(P("blk", "pix"), P("blk")),
        check_vma=False,
    )
```

```python
import functools

import jax
import jax.numpy as jnp
from jax import lax
from jax.experimental import pallas as pl
from jax.experimental.pallas import tpu as pltpu
from jax.sharding import PartitionSpec as P


BF16 = jnp.bfloat16
F32 = jnp.float32
MIB = 1 << 20
VMEM = pl.BlockSpec(memory_space=pltpu.VMEM)
SMEM = pl.BlockSpec(memory_space=pltpu.SMEM)
HBM = pl.BlockSpec(memory_space=pltpu.HBM)


def swap(value, axis, size, k):
    out = lax.ppermute(value, axis, [(i, i ^ k) for i in range(size)])
    return pltpu.with_memory_space_constraint(out, pltpu.VMEM)


def params(mib):
    return pltpu.CompilerParams(vmem_limit_bytes=mib * MIB)


def cost(flops, moved):
    return pl.CostEstimate(flops=int(flops), bytes_accessed=int(moved), transcendentals=0)


def prepare_kernel(order, rows, particles, ctf, noise, orient_class, class_prior, weighted, quadratic, prior, *scratch):
    p_buf, c_buf, n_buf, o_buf, r_buf, p_sem, c_sem, small_sem = scratch
    steps, tall, _ = p_buf.shape
    small = []
    for i, (source, target) in enumerate(((noise, n_buf), (orient_class, o_buf), (class_prior, r_buf))):
        small.append(pltpu.make_async_copy(source, target, small_sem.at[i]))
        small[-1].start()
    loads = []
    quarter = lax.axis_index("pix")
    lanes = prior.shape[1]
    for s in range(steps):
        first = (quarter ^ (s * tall // lanes)) * lanes + s * tall % lanes
        span = pl.ds(pl.multiple_of(first, tall), tall)
        a = pltpu.make_async_copy(particles.at[span], p_buf.at[s], p_sem.at[s])
        b = pltpu.make_async_copy(ctf.at[span], c_buf.at[s], c_sem.at[s])
        loads.append((a, b))
    ahead = min(4, steps)
    for a, b in loads[:ahead]:
        a.start()
        b.start()
    for copy in small:
        copy.wait()
    inverse = 1.0 / n_buf[...]
    orients = prior.shape[0]
    me = lax.axis_index("blk")
    classes = o_buf[...]
    table = jnp.zeros(classes.shape, F32)
    for c in range(r_buf.shape[1]):
        table = table + jnp.where(classes == c, r_buf[0:1, c : c + 1], jnp.float32(0.0))
    column = lax.broadcasted_iota(jnp.int32, (rows, orients), 1)
    row = lax.broadcasted_iota(jnp.int32, (rows, orients), 0)
    for slot, k in enumerate(order):
        hit = column == (me ^ k) * rows + row
        picked = jnp.sum(jnp.where(hit, table, jnp.float32(0.0)), axis=1, keepdims=True)
        prior[slot * rows : (slot + 1) * rows, :] = jnp.broadcast_to(picked, (rows, prior.shape[1]))
    for s, (a, b) in enumerate(loads):
        a.wait()
        b.wait()
        if s + ahead < steps:
            for copy in loads[s + ahead]:
                copy.start()
        span = slice(s * tall, (s + 1) * tall)
        wide = c_buf[s].astype(F32)
        scaled = wide * inverse
        weighted[span, :] = (p_buf[s].astype(F32) * scaled).astype(BF16)
        quadratic[span, :] = (wide * scaled).astype(BF16)


def prepare(order, rows, parts, particles, ctf, noise, orient_class, class_prior):
    slots, pixels = particles.shape
    steps = 2 * parts
    orients = orient_class.shape[1]
    operands = (particles, ctf, noise, orient_class, class_prior)
    return pl.pallas_call(
        functools.partial(prepare_kernel, order, rows),
        out_shape=(
            pltpu.VMEM((slots, pixels), BF16),
            pltpu.VMEM((slots, pixels), BF16),
            pltpu.VMEM((orients, slots // parts), F32),
        ),
        in_specs=[HBM] * 5,
        out_specs=(VMEM, VMEM, VMEM),
        scratch_shapes=[
            pltpu.VMEM((steps, slots // steps, pixels), BF16),
            pltpu.VMEM((steps, slots // steps, pixels), BF16),
            pltpu.VMEM((1, pixels), F32),
            pltpu.VMEM((1, orients), jnp.int32),
            pltpu.VMEM((1, class_prior.shape[1]), F32),
            pltpu.SemaphoreType.DMA((steps,)),
            pltpu.SemaphoreType.DMA((steps,)),
            pltpu.SemaphoreType.DMA((3,)),
        ],
        compiler_params=params(14),
        cost_estimate=cost(16 * slots * pixels, 8 * slots * pixels),
        name="prepare",
    )(*(pltpu.with_memory_space_constraint(value, pltpu.HBM) for value in operands))


def square_kernel(*refs):
    lines, square = refs[-2:]
    rows = refs[0].shape[0]
    for i, piece in enumerate(refs[:-2]):
        value = piece[...]
        wide = value.astype(F32)
        lines[i * rows : (i + 1) * rows, :] = value
        square[i * rows : (i + 1) * rows, :] = (-0.5 * wide * wide).astype(BF16)


def squares(proj):
    rows, pixels = proj[0].shape
    out = pltpu.VMEM((rows * len(proj), pixels), BF16)
    return pl.pallas_call(
        square_kernel,
        out_shape=(out, out),
        in_specs=[VMEM] * len(proj),
        out_specs=(VMEM, VMEM),
        compiler_params=params(4),
        cost_estimate=cost(1000 * rows * len(proj) * pixels, 6 * rows * len(proj) * pixels),
        name="squares",
    )(*proj)


NT = (((1,), (1,)), ((), ()))


def score_kernel(pieces, *refs):
    proj = refs[:pieces]
    lines, square, weighted, quadratic = refs[pieces : pieces + 4]
    *outs, lines_all, square_all = refs[pieces + 4 :]
    rows = proj[0].shape[0]
    first = lines.shape[0]
    lines_all[:first, :] = lines[...]
    square_all[:first, :] = square[...]
    for i, piece in enumerate(proj):
        value = piece[...]
        wide = value.astype(F32)
        span = slice(first + i * rows, first + (i + 1) * rows)
        lines_all[span, :] = value
        square_all[span, :] = (-0.5 * wide * wide).astype(BF16)
    lanes = outs[0].shape[1]
    total = lax.dot_general(weighted[2 * lanes :, :], lines_all[...], NT, preferred_element_type=F32) + lax.dot_general(
        quadratic[2 * lanes :, :], square_all[...], NT, preferred_element_type=F32
    )
    for j, out in enumerate(outs):
        out[...] = total[j * lanes : (j + 1) * lanes, :].T


def score(parts, proj, lines, square, weighted, quadratic):
    rows, pixels = proj[0].shape
    orients = rows * len(proj) + lines.shape[0]
    slots = weighted.shape[0]
    return pl.pallas_call(
        functools.partial(score_kernel, len(proj)),
        out_shape=tuple(pltpu.VMEM((orients, slots // parts), F32) for _ in range(parts - 2))
        + (pltpu.VMEM((orients, pixels), BF16),) * 2,
        in_specs=[VMEM] * (len(proj) + 4),
        out_specs=(VMEM,) * parts,
        compiler_params=params(12),
        cost_estimate=cost(4 * orients * slots * pixels, 4 * slots * pixels),
        name="score",
    )(*proj, lines, square, weighted, quadratic)


def own_kernel(base, lines, square, weighted, quadratic, out):
    lanes = out.shape[1]
    held = slice(base * lanes, (base + 1) * lanes)
    total = lax.dot_general(weighted[held, :], lines[...], NT, preferred_element_type=F32) + lax.dot_general(
        quadratic[held, :], square[...], NT, preferred_element_type=F32
    )
    out[...] = total.T


def own_score(parts, base, lines, square, weighted, quadratic):
    orients, pixels = lines.shape
    lanes = weighted.shape[0] // parts
    return pl.pallas_call(
        functools.partial(own_kernel, base),
        out_shape=pltpu.VMEM((orients, lanes), F32),
        in_specs=[VMEM] * 4,
        out_specs=VMEM,
        compiler_params=params(12),
        cost_estimate=cost(4 * orients * lanes * pixels, 4 * lanes * pixels),
        name="own_score",
    )(lines, square, weighted, quadratic)


def weigh_kernel(parts, *refs):
    prior, counts = refs[parts : parts + 2]
    out = refs[parts + 2]
    logits = refs[0][...]
    for piece in refs[1:parts]:
        logits = logits + piece[...]
    logits = logits + prior[...]
    orients, lanes = logits.shape
    peak = jnp.max(logits, axis=0, keepdims=True)
    log_total = peak + jnp.log(jnp.sum(jnp.exp(logits - peak), axis=0, keepdims=True))
    slot = lax.axis_index("pix") * lanes + lax.broadcasted_iota(jnp.int32, (1, lanes), 1)
    live = slot < counts[0]
    out[:orients, :] = jnp.where(live, jnp.exp(logits - log_total), jnp.float32(0.0)).astype(BF16)
    norm = jnp.where(live, log_total, jnp.float32(0.0))
    high = norm.astype(BF16).astype(F32)
    rest = norm - high
    middle = rest.astype(BF16).astype(F32)
    low = rest - middle
    line = lax.broadcasted_iota(jnp.int32, (16, lanes), 0)
    tail = jnp.where(line == 0, high, jnp.where(line == 1, middle, jnp.where(line == 2, low, jnp.float32(0.0))))
    out[orients:, :] = tail.astype(BF16)


def weigh(pieces, prior, counts):
    orients, lanes = prior.shape
    return pl.pallas_call(
        functools.partial(weigh_kernel, len(pieces)),
        out_shape=pltpu.VMEM((orients + 16, lanes), BF16),
        in_specs=[VMEM] * (len(pieces) + 1) + [SMEM],
        out_specs=VMEM,
        compiler_params=params(8),
        cost_estimate=cost(40 * orients * lanes, 20 * orients * lanes),
        name="weigh",
    )(*pieces, prior, counts)


def field_kernel(parts, *refs):
    pieces = refs[:parts]
    weighted, kept, sent, late, norm, lhs = refs[parts:]
    orients, slots = lhs.shape
    lanes = slots // parts
    quarter = lax.axis_index("pix")
    for j, piece in enumerate(pieces):
        place = quarter ^ j
        lhs[:, j * lanes : (j + 1) * lanes] = piece[:orients, :]
        tail = piece[orients:, :].astype(F32)
        norm[pl.ds(place, 1), :] = (tail[0:1] + tail[1:2]) + tail[2:3]
    half = orients // 2
    pixels = weighted.shape[1]
    wide = 1024 if pixels % 1024 == 0 else pixels
    for c in range(pixels // wide):
        span = slice(c * wide, (c + 1) * wide)
        value = jnp.dot(lhs[...], weighted[:, span], preferred_element_type=F32)
        kept[:, span] = value[:half]
        rest = value[half:].astype(BF16)
        sent[:, span] = rest[: sent.shape[0]]
        late[:, span] = rest[sent.shape[0] :]


def field(pieces, weighted, first):
    slots, pixels = weighted.shape
    parts = len(pieces)
    orients = pieces[0].shape[0] - 16
    return pl.pallas_call(
        functools.partial(field_kernel, parts),
        out_shape=(
            pltpu.VMEM((orients // 2, pixels), F32),
            pltpu.VMEM((first, pixels), BF16),
            pltpu.VMEM((orients // 2 - first, pixels), BF16),
            pltpu.VMEM((parts, slots // parts), F32),
        ),
        in_specs=[VMEM] * (parts + 1),
        out_specs=(VMEM,) * 4,
        scratch_shapes=[pltpu.VMEM((orients, slots), BF16)],
        compiler_params=params(16),
        cost_estimate=cost(2 * orients * slots * pixels, 2 * slots * pixels),
        name="field",
    )(*pieces, weighted)


def pair_kernel(base, kept, got, *outs):
    rows = outs[0].shape[0]
    for i, out in enumerate(outs):
        span = slice(i * rows, (i + 1) * rows)
        mine = slice(base + i * rows, base + (i + 1) * rows)
        out[...] = (kept[mine, :] + got[span, :].astype(F32)).astype(out.dtype)


def pair(kept, got, rows, base, types):
    orients, pixels = got.shape
    return pl.pallas_call(
        functools.partial(pair_kernel, base),
        out_shape=tuple(pltpu.VMEM((rows, pixels), kind) for kind in types),
        in_specs=[VMEM, VMEM],
        out_specs=(VMEM,) * len(types),
        compiler_params=params(8),
        cost_estimate=cost(2 * orients * pixels, 8 * orients * pixels),
        name="pair",
    )(kept, got)


def final_kernel(own, *refs):
    total = own[...]
    for piece in refs[:-1]:
        total = total + piece[...].astype(F32)
    refs[-1][...] = total


def final(own, pieces):
    return pl.pallas_call(
        final_kernel,
        out_shape=jax.ShapeDtypeStruct(own.shape, F32),
        in_specs=[VMEM] * (len(pieces) + 1),
        out_specs=VMEM,
        compiler_params=params(16),
        cost_estimate=cost(own.size * len(pieces), 4 * own.size * len(pieces)),
        name="final",
    )(own, *pieces)


def body(blk, pix, particles, ctf, noise_var, projections, orient_class, class_prior, counts):
    rows = projections.shape[0]
    even = list(range(2, blk, 2))
    lead = even[:-1] + [0] + even[-1:]
    order = lead + [k ^ 1 for k in lead]
    noise, orient_class, class_prior = (value.reshape(1, -1) for value in (noise_var, orient_class, class_prior))
    far = {0: projections}
    near = {}
    for k in even:
        far[k] = swap(projections, "blk", blk, k)
    near[0] = swap(projections, "blk", blk, 1)
    weighted, quadratic, prior = prepare(order, rows, pix, particles, ctf, noise, orient_class, class_prior)
    for k in even:
        near[k] = swap(far[k], "blk", blk, 1)
    lines, square = squares([far[k] for k in lead])
    *chunks, lines, square = score(pix, [near[k] for k in lead], lines, square, weighted, quadratic)
    pieces = []
    for j in range(2, pix):
        pieces.append(swap(chunks[j - 2], "pix", pix, j))
    beside = own_score(pix, 1, lines, square, weighted, quadratic)
    pieces.append(swap(beside, "pix", pix, 1))
    pieces.insert(0, own_score(pix, 0, lines, square, weighted, quadratic))
    weights = weigh(pieces, prior, counts)
    parts = [weights]
    for j in range(1, pix):
        parts.append(swap(weights, "pix", pix, j))
    first = rows * (len(lead) - 2)
    kept, sent, late, norm = field(parts, weighted, first)
    sent = swap(sent, "blk", blk, 1)
    late = swap(late, "blk", blk, 1)
    out = list(pair(kept, sent, rows, 0, [BF16] * (len(lead) - 2)))
    own, last = pair(kept, late, rows, first, [F32, BF16])
    got = []
    for piece, k in zip(out + [last], even):
        got.append(swap(piece, "blk", blk, k))
    return final(own, got), norm.reshape(-1)


def solution(mesh):
    placed = (P("blk", "pix"), P("blk", "pix"), P("pix"), P("blk", "pix"), P(), P(), P("blk"))
    return jax.shard_map(
        functools.partial(body, mesh.shape["blk"], mesh.shape["pix"]),
        mesh=mesh,
        in_specs=placed,
        out_specs=(P("blk", "pix"), P("blk")),
        check_vma=False,
    )
```

```python
import functools

import jax
import jax.numpy as jnp
from jax import lax
from jax.experimental import pallas as pl
from jax.experimental.pallas import tpu as pltpu
from jax.sharding import PartitionSpec as P


BF16 = jnp.bfloat16
F32 = jnp.float32
MIB = 1 << 20
VMEM = pl.BlockSpec(memory_space=pltpu.VMEM)
SMEM = pl.BlockSpec(memory_space=pltpu.SMEM)
HBM = pl.BlockSpec(memory_space=pltpu.HBM)


def swap(value, axis, size, k):
    out = lax.ppermute(value, axis, [(i, i ^ k) for i in range(size)])
    return pltpu.with_memory_space_constraint(out, pltpu.VMEM)


def params(mib):
    return pltpu.CompilerParams(vmem_limit_bytes=mib * MIB)


def cost(flops, moved):
    return pl.CostEstimate(flops=int(flops), bytes_accessed=int(moved), transcendentals=0)


def prepare_kernel(order, rows, particles, ctf, noise, orient_class, class_prior, weighted, quadratic, prior, *scratch):
    p_buf, c_buf, n_buf, o_buf, r_buf, p_sem, c_sem, small_sem = scratch
    steps, tall, _ = p_buf.shape
    small = []
    for i, (source, target) in enumerate(((noise, n_buf), (orient_class, o_buf), (class_prior, r_buf))):
        small.append(pltpu.make_async_copy(source, target, small_sem.at[i]))
        small[-1].start()
    loads = []
    quarter = lax.axis_index("pix")
    lanes = prior.shape[1]
    for s in range(steps):
        first = (quarter ^ (s * tall // lanes)) * lanes + s * tall % lanes
        span = pl.ds(pl.multiple_of(first, tall), tall)
        a = pltpu.make_async_copy(particles.at[span], p_buf.at[s], p_sem.at[s])
        b = pltpu.make_async_copy(ctf.at[span], c_buf.at[s], c_sem.at[s])
        loads.append((a, b))
    ahead = min(4, steps)
    for a, b in loads[:ahead]:
        a.start()
        b.start()
    for copy in small:
        copy.wait()
    inverse = 1.0 / n_buf[...]
    orients = prior.shape[0]
    me = lax.axis_index("blk")
    classes = o_buf[...]
    table = jnp.zeros(classes.shape, F32)
    for c in range(r_buf.shape[1]):
        table = table + jnp.where(classes == c, r_buf[0:1, c : c + 1], jnp.float32(0.0))
    column = lax.broadcasted_iota(jnp.int32, (rows, orients), 1)
    row = lax.broadcasted_iota(jnp.int32, (rows, orients), 0)
    for slot, k in enumerate(order):
        hit = column == (me ^ k) * rows + row
        picked = jnp.sum(jnp.where(hit, table, jnp.float32(0.0)), axis=1, keepdims=True)
        prior[slot * rows : (slot + 1) * rows, :] = jnp.broadcast_to(picked, (rows, prior.shape[1]))
    for s, (a, b) in enumerate(loads):
        a.wait()
        b.wait()
        if s + ahead < steps:
            for copy in loads[s + ahead]:
                copy.start()
        span = slice(s * tall, (s + 1) * tall)
        wide = c_buf[s].astype(F32)
        scaled = wide * inverse
        weighted[span, :] = (p_buf[s].astype(F32) * scaled).astype(BF16)
        quadratic[span, :] = (wide * scaled).astype(BF16)


def prepare(order, rows, parts, particles, ctf, noise, orient_class, class_prior):
    slots, pixels = particles.shape
    steps = 2 * parts
    orients = orient_class.shape[1]
    operands = (particles, ctf, noise, orient_class, class_prior)
    return pl.pallas_call(
        functools.partial(prepare_kernel, order, rows),
        out_shape=(
            pltpu.VMEM((slots, pixels), BF16),
            pltpu.VMEM((slots, pixels), BF16),
            pltpu.VMEM((orients, slots // parts), F32),
        ),
        in_specs=[HBM] * 5,
        out_specs=(VMEM, VMEM, VMEM),
        scratch_shapes=[
            pltpu.VMEM((steps, slots // steps, pixels), BF16),
            pltpu.VMEM((steps, slots // steps, pixels), BF16),
            pltpu.VMEM((1, pixels), F32),
            pltpu.VMEM((1, orients), jnp.int32),
            pltpu.VMEM((1, class_prior.shape[1]), F32),
            pltpu.SemaphoreType.DMA((steps,)),
            pltpu.SemaphoreType.DMA((steps,)),
            pltpu.SemaphoreType.DMA((3,)),
        ],
        compiler_params=params(14),
        cost_estimate=cost(16 * slots * pixels, 8 * slots * pixels),
        name="prepare",
    )(*(pltpu.with_memory_space_constraint(value, pltpu.HBM) for value in operands))


def square_kernel(*refs):
    lines, square = refs[-2:]
    rows = refs[0].shape[0]
    for i, piece in enumerate(refs[:-2]):
        value = piece[...]
        wide = value.astype(F32)
        lines[i * rows : (i + 1) * rows, :] = value
        square[i * rows : (i + 1) * rows, :] = (-0.5 * wide * wide).astype(BF16)


def squares(proj):
    rows, pixels = proj[0].shape
    out = pltpu.VMEM((rows * len(proj), pixels), BF16)
    return pl.pallas_call(
        square_kernel,
        out_shape=(out, out),
        in_specs=[VMEM] * len(proj),
        out_specs=(VMEM, VMEM),
        compiler_params=params(4),
        cost_estimate=cost(1000 * rows * len(proj) * pixels, 6 * rows * len(proj) * pixels),
        name="squares",
    )(*proj)


NT = (((1,), (1,)), ((), ()))


def score_kernel(pieces, *refs):
    proj = refs[:pieces]
    lines, square, weighted, quadratic = refs[pieces : pieces + 4]
    *outs, lines_all, square_all = refs[pieces + 4 :]
    rows = proj[0].shape[0]
    first = lines.shape[0]
    lines_all[:first, :] = lines[...]
    square_all[:first, :] = square[...]
    for i, piece in enumerate(proj):
        value = piece[...]
        wide = value.astype(F32)
        span = slice(first + i * rows, first + (i + 1) * rows)
        lines_all[span, :] = value
        square_all[span, :] = (-0.5 * wide * wide).astype(BF16)
    lanes = outs[0].shape[1]
    total = lax.dot_general(weighted[2 * lanes :, :], lines_all[...], NT, preferred_element_type=F32) + lax.dot_general(
        quadratic[2 * lanes :, :], square_all[...], NT, preferred_element_type=F32
    )
    for j, out in enumerate(outs):
        out[...] = total[j * lanes : (j + 1) * lanes, :].T


def score(parts, proj, lines, square, weighted, quadratic):
    rows, pixels = proj[0].shape
    orients = rows * len(proj) + lines.shape[0]
    slots = weighted.shape[0]
    return pl.pallas_call(
        functools.partial(score_kernel, len(proj)),
        out_shape=tuple(pltpu.VMEM((orients, slots // parts), F32) for _ in range(parts - 2))
        + (pltpu.VMEM((orients, pixels), BF16),) * 2,
        in_specs=[VMEM] * (len(proj) + 4),
        out_specs=(VMEM,) * parts,
        compiler_params=params(12),
        cost_estimate=cost(4 * orients * slots * pixels, 4 * slots * pixels),
        name="score",
    )(*proj, lines, square, weighted, quadratic)


def own_kernel(base, lines, square, weighted, quadratic, out):
    lanes = out.shape[1]
    held = slice(base * lanes, (base + 1) * lanes)
    total = lax.dot_general(weighted[held, :], lines[...], NT, preferred_element_type=F32) + lax.dot_general(
        quadratic[held, :], square[...], NT, preferred_element_type=F32
    )
    out[...] = total.T


def own_score(parts, base, lines, square, weighted, quadratic):
    orients, pixels = lines.shape
    lanes = weighted.shape[0] // parts
    return pl.pallas_call(
        functools.partial(own_kernel, base),
        out_shape=pltpu.VMEM((orients, lanes), F32),
        in_specs=[VMEM] * 4,
        out_specs=VMEM,
        compiler_params=params(12),
        cost_estimate=cost(4 * orients * lanes * pixels, 4 * lanes * pixels),
        name="own_score",
    )(lines, square, weighted, quadratic)


def weigh_kernel(parts, *refs):
    prior, counts = refs[parts : parts + 2]
    out = refs[parts + 2]
    logits = refs[0][...]
    for piece in refs[1:parts]:
        logits = logits + piece[...]
    logits = logits + prior[...]
    orients, lanes = logits.shape
    peak = jnp.max(logits, axis=0, keepdims=True)
    log_total = peak + jnp.log(jnp.sum(jnp.exp(logits - peak), axis=0, keepdims=True))
    slot = lax.axis_index("pix") * lanes + lax.broadcasted_iota(jnp.int32, (1, lanes), 1)
    live = slot < counts[0]
    out[:orients, :] = jnp.where(live, jnp.exp(logits - log_total), jnp.float32(0.0)).astype(BF16)
    norm = jnp.where(live, log_total, jnp.float32(0.0))
    high = norm.astype(BF16).astype(F32)
    rest = norm - high
    middle = rest.astype(BF16).astype(F32)
    low = rest - middle
    line = lax.broadcasted_iota(jnp.int32, (16, lanes), 0)
    tail = jnp.where(line == 0, high, jnp.where(line == 1, middle, jnp.where(line == 2, low, jnp.float32(0.0))))
    out[orients:, :] = tail.astype(BF16)


def weigh(pieces, prior, counts):
    orients, lanes = prior.shape
    return pl.pallas_call(
        functools.partial(weigh_kernel, len(pieces)),
        out_shape=pltpu.VMEM((orients + 16, lanes), BF16),
        in_specs=[VMEM] * (len(pieces) + 1) + [SMEM],
        out_specs=VMEM,
        compiler_params=params(8),
        cost_estimate=cost(40 * orients * lanes, 20 * orients * lanes),
        name="weigh",
    )(*pieces, prior, counts)


def field_kernel(parts, *refs):
    pieces = refs[:parts]
    weighted, kept, sent, late, norm, lhs = refs[parts:]
    orients, slots = lhs.shape
    lanes = slots // parts
    quarter = lax.axis_index("pix")
    for j, piece in enumerate(pieces):
        place = quarter ^ j
        lhs[:, j * lanes : (j + 1) * lanes] = piece[:orients, :]
        tail = piece[orients:, :].astype(F32)
        norm[pl.ds(place, 1), :] = (tail[0:1] + tail[1:2]) + tail[2:3]
    half = orients // 2
    pixels = weighted.shape[1]
    wide = 1024 if pixels % 1024 == 0 else pixels
    for c in range(pixels // wide):
        span = slice(c * wide, (c + 1) * wide)
        value = jnp.dot(lhs[...], weighted[:, span], preferred_element_type=F32)
        kept[:, span] = value[:half]
        rest = value[half:].astype(BF16)
        sent[:, span] = rest[: sent.shape[0]]
        late[:, span] = rest[sent.shape[0] :]


def field(pieces, weighted, first):
    slots, pixels = weighted.shape
    parts = len(pieces)
    orients = pieces[0].shape[0] - 16
    return pl.pallas_call(
        functools.partial(field_kernel, parts),
        out_shape=(
            pltpu.VMEM((orients // 2, pixels), F32),
            pltpu.VMEM((first, pixels), BF16),
            pltpu.VMEM((orients // 2 - first, pixels), BF16),
            pltpu.VMEM((parts, slots // parts), F32),
        ),
        in_specs=[VMEM] * (parts + 1),
        out_specs=(VMEM,) * 4,
        scratch_shapes=[pltpu.VMEM((orients, slots), BF16)],
        compiler_params=params(16),
        cost_estimate=cost(2 * orients * slots * pixels, 2 * slots * pixels),
        name="field",
    )(*pieces, weighted)


def pair_kernel(base, kept, got, *outs):
    rows = outs[0].shape[0]
    for i, out in enumerate(outs):
        span = slice(i * rows, (i + 1) * rows)
        mine = slice(base + i * rows, base + (i + 1) * rows)
        out[...] = (kept[mine, :] + got[span, :].astype(F32)).astype(out.dtype)


def pair(kept, got, rows, base, types):
    orients, pixels = got.shape
    return pl.pallas_call(
        functools.partial(pair_kernel, base),
        out_shape=tuple(pltpu.VMEM((rows, pixels), kind) for kind in types),
        in_specs=[VMEM, VMEM],
        out_specs=(VMEM,) * len(types),
        compiler_params=params(8),
        cost_estimate=cost(2 * orients * pixels, 8 * orients * pixels),
        name="pair",
    )(kept, got)


def final_kernel(own, *refs):
    *pieces, out, held, sems = refs
    copies = []
    for i, span in enumerate(spans(own.shape[1])):
        total = own[:, span]
        for piece in pieces:
            total = total + piece[:, span].astype(F32)
        held[:, span] = total
        copies.append(pltpu.make_async_copy(held.at[:, span], out.at[:, span], sems.at[i]))
        copies[-1].start()
    for copy in copies:
        copy.wait()


def spans(pixels):
    wide = pixels // 4 if pixels % 512 == 0 else pixels
    return [slice(c * wide, (c + 1) * wide) for c in range(pixels // wide)]


def final(own, pieces):
    return pl.pallas_call(
        final_kernel,
        out_shape=jax.ShapeDtypeStruct(own.shape, F32),
        in_specs=[VMEM] * (len(pieces) + 1),
        out_specs=HBM,
        scratch_shapes=[pltpu.VMEM(own.shape, F32), pltpu.SemaphoreType.DMA((len(spans(own.shape[1])),))],
        compiler_params=params(16),
        cost_estimate=cost(own.size * len(pieces), 4 * own.size * len(pieces)),
        name="final",
    )(own, *pieces)


def body(blk, pix, particles, ctf, noise_var, projections, orient_class, class_prior, counts):
    rows = projections.shape[0]
    even = list(range(2, blk, 2))
    lead = even[:-1] + [0] + even[-1:]
    order = lead + [k ^ 1 for k in lead]
    noise, orient_class, class_prior = (value.reshape(1, -1) for value in (noise_var, orient_class, class_prior))
    far = {0: projections}
    near = {}
    for k in even:
        far[k] = swap(projections, "blk", blk, k)
    near[0] = swap(projections, "blk", blk, 1)
    weighted, quadratic, prior = prepare(order, rows, pix, particles, ctf, noise, orient_class, class_prior)
    for k in even:
        near[k] = swap(far[k], "blk", blk, 1)
    lines, square = squares([far[k] for k in lead])
    *chunks, lines, square = score(pix, [near[k] for k in lead], lines, square, weighted, quadratic)
    pieces = []
    for j in range(2, pix):
        pieces.append(swap(chunks[j - 2], "pix", pix, j))
    beside = own_score(pix, 1, lines, square, weighted, quadratic)
    pieces.append(swap(beside, "pix", pix, 1))
    pieces.insert(0, own_score(pix, 0, lines, square, weighted, quadratic))
    weights = weigh(pieces, prior, counts)
    parts = [weights]
    for j in range(1, pix):
        parts.append(swap(weights, "pix", pix, j))
    first = rows * (len(lead) - 2)
    kept, sent, late, norm = field(parts, weighted, first)
    sent = swap(sent, "blk", blk, 1)
    late = swap(late, "blk", blk, 1)
    out = list(pair(kept, sent, rows, 0, [BF16] * (len(lead) - 2)))
    own, last = pair(kept, late, rows, first, [F32, BF16])
    got = []
    for piece, k in zip(out + [last], even):
        got.append(swap(piece, "blk", blk, k))
    return final(own, got), norm.reshape(-1)


def solution(mesh):
    placed = (P("blk", "pix"), P("blk", "pix"), P("pix"), P("blk", "pix"), P(), P(), P("blk"))
    return jax.shard_map(
        functools.partial(body, mesh.shape["blk"], mesh.shape["pix"]),
        mesh=mesh,
        in_specs=placed,
        out_specs=(P("blk", "pix"), P("blk")),
        check_vma=False,
    )
```

```python
import functools

import jax
import jax.numpy as jnp
from jax import lax
from jax.experimental import pallas as pl
from jax.experimental.pallas import tpu as pltpu
from jax.sharding import PartitionSpec as P


BF16 = jnp.bfloat16
F32 = jnp.float32
MIB = 1 << 20
VMEM = pl.BlockSpec(memory_space=pltpu.VMEM)
SMEM = pl.BlockSpec(memory_space=pltpu.SMEM)
HBM = pl.BlockSpec(memory_space=pltpu.HBM)


def swap(value, axis, size, k):
    out = lax.ppermute(value, axis, [(i, i ^ k) for i in range(size)])
    return pltpu.with_memory_space_constraint(out, pltpu.VMEM)


def params(mib):
    return pltpu.CompilerParams(vmem_limit_bytes=mib * MIB)


def cost(flops, moved):
    return pl.CostEstimate(flops=int(flops), bytes_accessed=int(moved), transcendentals=0)


def prepare_kernel(order, rows, particles, ctf, noise, orient_class, class_prior, weighted, quadratic, prior, *scratch):
    p_buf, c_buf, n_buf, o_buf, r_buf, p_sem, c_sem, small_sem = scratch
    steps, tall, _ = p_buf.shape
    small = []
    for i, (source, target) in enumerate(((noise, n_buf), (orient_class, o_buf), (class_prior, r_buf))):
        small.append(pltpu.make_async_copy(source, target, small_sem.at[i]))
        small[-1].start()
    loads = []
    quarter = lax.axis_index("pix")
    lanes = prior.shape[1]
    for s in range(steps):
        first = (quarter ^ (s * tall // lanes)) * lanes + s * tall % lanes
        span = pl.ds(pl.multiple_of(first, tall), tall)
        a = pltpu.make_async_copy(particles.at[span], p_buf.at[s], p_sem.at[s])
        b = pltpu.make_async_copy(ctf.at[span], c_buf.at[s], c_sem.at[s])
        loads.append((a, b))
    ahead = min(4, steps)
    for a, b in loads[:ahead]:
        a.start()
        b.start()
    for copy in small:
        copy.wait()
    inverse = 1.0 / n_buf[...]
    orients = prior.shape[0]
    me = lax.axis_index("blk")
    classes = o_buf[...]
    table = jnp.zeros(classes.shape, F32)
    for c in range(r_buf.shape[1]):
        table = table + jnp.where(classes == c, r_buf[0:1, c : c + 1], jnp.float32(0.0))
    column = lax.broadcasted_iota(jnp.int32, (rows, orients), 1)
    row = lax.broadcasted_iota(jnp.int32, (rows, orients), 0)
    for slot, k in enumerate(order):
        hit = column == (me ^ k) * rows + row
        picked = jnp.sum(jnp.where(hit, table, jnp.float32(0.0)), axis=1, keepdims=True)
        prior[slot * rows : (slot + 1) * rows, :] = jnp.broadcast_to(picked, (rows, prior.shape[1]))
    for s, (a, b) in enumerate(loads):
        a.wait()
        b.wait()
        if s + ahead < steps:
            for copy in loads[s + ahead]:
                copy.start()
        span = slice(s * tall, (s + 1) * tall)
        wide = c_buf[s].astype(F32)
        scaled = wide * inverse
        weighted[span, :] = (p_buf[s].astype(F32) * scaled).astype(BF16)
        quadratic[span, :] = (wide * scaled).astype(BF16)


def prepare(order, rows, parts, particles, ctf, noise, orient_class, class_prior):
    slots, pixels = particles.shape
    steps = 2 * parts
    orients = orient_class.shape[1]
    operands = (particles, ctf, noise, orient_class, class_prior)
    return pl.pallas_call(
        functools.partial(prepare_kernel, order, rows),
        out_shape=(
            pltpu.VMEM((slots, pixels), BF16),
            pltpu.VMEM((slots, pixels), BF16),
            pltpu.VMEM((orients, slots // parts), F32),
        ),
        in_specs=[HBM] * 5,
        out_specs=(VMEM, VMEM, VMEM),
        scratch_shapes=[
            pltpu.VMEM((steps, slots // steps, pixels), BF16),
            pltpu.VMEM((steps, slots // steps, pixels), BF16),
            pltpu.VMEM((1, pixels), F32),
            pltpu.VMEM((1, orients), jnp.int32),
            pltpu.VMEM((1, class_prior.shape[1]), F32),
            pltpu.SemaphoreType.DMA((steps,)),
            pltpu.SemaphoreType.DMA((steps,)),
            pltpu.SemaphoreType.DMA((3,)),
        ],
        compiler_params=params(14),
        cost_estimate=cost(16 * slots * pixels, 8 * slots * pixels),
        name="prepare",
    )(*(pltpu.with_memory_space_constraint(value, pltpu.HBM) for value in operands))


def square_kernel(*refs):
    lines, square = refs[-2:]
    rows = refs[0].shape[0]
    for i, piece in enumerate(refs[:-2]):
        value = piece[...]
        wide = value.astype(F32)
        lines[i * rows : (i + 1) * rows, :] = value
        square[i * rows : (i + 1) * rows, :] = (-0.5 * wide * wide).astype(BF16)


def squares(proj):
    rows, pixels = proj[0].shape
    out = pltpu.VMEM((rows * len(proj), pixels), BF16)
    return pl.pallas_call(
        square_kernel,
        out_shape=(out, out),
        in_specs=[VMEM] * len(proj),
        out_specs=(VMEM, VMEM),
        compiler_params=params(4),
        cost_estimate=cost(1000 * rows * len(proj) * pixels, 6 * rows * len(proj) * pixels),
        name="squares",
    )(*proj)


NT = (((1,), (1,)), ((), ()))


def score_kernel(pieces, *refs):
    proj = refs[:pieces]
    lines, square, weighted, quadratic = refs[pieces : pieces + 4]
    *outs, lines_all, square_all = refs[pieces + 4 :]
    rows = proj[0].shape[0]
    first = lines.shape[0]
    lines_all[:first, :] = lines[...]
    square_all[:first, :] = square[...]
    for i, piece in enumerate(proj):
        value = piece[...]
        wide = value.astype(F32)
        span = slice(first + i * rows, first + (i + 1) * rows)
        lines_all[span, :] = value
        square_all[span, :] = (-0.5 * wide * wide).astype(BF16)
    lanes = outs[0].shape[1]
    total = lax.dot_general(weighted[2 * lanes :, :], lines_all[...], NT, preferred_element_type=F32) + lax.dot_general(
        quadratic[2 * lanes :, :], square_all[...], NT, preferred_element_type=F32
    )
    for j, out in enumerate(outs):
        out[...] = total[j * lanes : (j + 1) * lanes, :].T


def score(parts, proj, lines, square, weighted, quadratic):
    rows, pixels = proj[0].shape
    orients = rows * len(proj) + lines.shape[0]
    slots = weighted.shape[0]
    return pl.pallas_call(
        functools.partial(score_kernel, len(proj)),
        out_shape=tuple(pltpu.VMEM((orients, slots // parts), F32) for _ in range(parts - 2))
        + (pltpu.VMEM((orients, pixels), BF16),) * 2,
        in_specs=[VMEM] * (len(proj) + 4),
        out_specs=(VMEM,) * parts,
        compiler_params=params(12),
        cost_estimate=cost(4 * orients * slots * pixels, 4 * slots * pixels),
        name="score",
    )(*proj, lines, square, weighted, quadratic)


def own_kernel(base, lines, square, weighted, quadratic, out):
    lanes = out.shape[1]
    held = slice(base * lanes, (base + 1) * lanes)
    total = lax.dot_general(weighted[held, :], lines[...], NT, preferred_element_type=F32) + lax.dot_general(
        quadratic[held, :], square[...], NT, preferred_element_type=F32
    )
    out[...] = total.T


def own_score(parts, base, lines, square, weighted, quadratic):
    orients, pixels = lines.shape
    lanes = weighted.shape[0] // parts
    return pl.pallas_call(
        functools.partial(own_kernel, base),
        out_shape=pltpu.VMEM((orients, lanes), F32),
        in_specs=[VMEM] * 4,
        out_specs=VMEM,
        compiler_params=params(12),
        cost_estimate=cost(4 * orients * lanes * pixels, 4 * lanes * pixels),
        name="own_score",
    )(lines, square, weighted, quadratic)


def weigh_kernel(parts, *refs):
    prior, counts = refs[parts : parts + 2]
    out = refs[parts + 2]
    logits = refs[0][...]
    for piece in refs[1:parts]:
        logits = logits + piece[...]
    logits = logits + prior[...]
    orients, lanes = logits.shape
    peak = jnp.max(logits, axis=0, keepdims=True)
    log_total = peak + jnp.log(jnp.sum(jnp.exp(logits - peak), axis=0, keepdims=True))
    slot = lax.axis_index("pix") * lanes + lax.broadcasted_iota(jnp.int32, (1, lanes), 1)
    live = slot < counts[0]
    out[:orients, :] = jnp.where(live, jnp.exp(logits - log_total), jnp.float32(0.0)).astype(BF16)
    norm = jnp.where(live, log_total, jnp.float32(0.0))
    high = norm.astype(BF16).astype(F32)
    rest = norm - high
    middle = rest.astype(BF16).astype(F32)
    low = rest - middle
    line = lax.broadcasted_iota(jnp.int32, (16, lanes), 0)
    tail = jnp.where(line == 0, high, jnp.where(line == 1, middle, jnp.where(line == 2, low, jnp.float32(0.0))))
    out[orients:, :] = tail.astype(BF16)


def weigh(pieces, prior, counts):
    orients, lanes = prior.shape
    return pl.pallas_call(
        functools.partial(weigh_kernel, len(pieces)),
        out_shape=pltpu.VMEM((orients + 16, lanes), BF16),
        in_specs=[VMEM] * (len(pieces) + 1) + [SMEM],
        out_specs=VMEM,
        compiler_params=params(8),
        cost_estimate=cost(40 * orients * lanes, 20 * orients * lanes),
        name="weigh",
    )(*pieces, prior, counts)


def field_kernel(parts, *refs):
    pieces = refs[:parts]
    weighted, kept, sent, late, norm, lhs = refs[parts:]
    orients, slots = lhs.shape
    lanes = slots // parts
    quarter = lax.axis_index("pix")
    for j, piece in enumerate(pieces):
        place = quarter ^ j
        lhs[:, j * lanes : (j + 1) * lanes] = piece[:orients, :]
        tail = piece[orients:, :].astype(F32)
        norm[pl.ds(place, 1), :] = (tail[0:1] + tail[1:2]) + tail[2:3]
    half = orients // 2
    pixels = weighted.shape[1]
    wide = 1024 if pixels % 1024 == 0 else pixels
    for c in range(pixels // wide):
        span = slice(c * wide, (c + 1) * wide)
        value = jnp.dot(lhs[...], weighted[:, span], preferred_element_type=F32)
        kept[:, span] = value[:half]
        rest = value[half:].astype(BF16)
        sent[:, span] = rest[: sent.shape[0]]
        late[:, span] = rest[sent.shape[0] :]


def field(pieces, weighted, first):
    slots, pixels = weighted.shape
    parts = len(pieces)
    orients = pieces[0].shape[0] - 16
    return pl.pallas_call(
        functools.partial(field_kernel, parts),
        out_shape=(
            pltpu.VMEM((orients // 2, pixels), F32),
            pltpu.VMEM((first, pixels), BF16),
            pltpu.VMEM((orients // 2 - first, pixels), BF16),
            pltpu.VMEM((parts, slots // parts), F32),
        ),
        in_specs=[VMEM] * (parts + 1),
        out_specs=(VMEM,) * 4,
        scratch_shapes=[pltpu.VMEM((orients, slots), BF16)],
        compiler_params=params(16),
        cost_estimate=cost(2 * orients * slots * pixels, 2 * slots * pixels),
        name="field",
    )(*pieces, weighted)


def pair_kernel(base, kept, got, *outs):
    rows = outs[0].shape[0]
    for i, out in enumerate(outs):
        span = slice(i * rows, (i + 1) * rows)
        mine = slice(base + i * rows, base + (i + 1) * rows)
        out[...] = (kept[mine, :] + got[span, :].astype(F32)).astype(out.dtype)


def pair(kept, got, rows, base, types):
    orients, pixels = got.shape
    return pl.pallas_call(
        functools.partial(pair_kernel, base),
        out_shape=tuple(pltpu.VMEM((rows, pixels), kind) for kind in types),
        in_specs=[VMEM, VMEM],
        out_specs=(VMEM,) * len(types),
        compiler_params=params(8),
        cost_estimate=cost(2 * orients * pixels, 8 * orients * pixels),
        name="pair",
    )(kept, got)


def final_kernel(own, *refs):
    *pieces, out, held, sems = refs
    copies = []
    for i, span in enumerate(spans(own.shape[1])):
        total = own[:, span]
        for piece in pieces:
            total = total + piece[:, span].astype(F32)
        held[:, span] = total
        copies.append(pltpu.make_async_copy(held.at[:, span], out.at[:, span], sems.at[i]))
        copies[-1].start()
    for copy in copies:
        copy.wait()


def spans(pixels):
    wide = pixels // 4 if pixels % 512 == 0 else pixels
    return [slice(c * wide, (c + 1) * wide) for c in range(pixels // wide)]


def final(own, pieces):
    return pl.pallas_call(
        final_kernel,
        out_shape=jax.ShapeDtypeStruct(own.shape, F32),
        in_specs=[VMEM] * (len(pieces) + 1),
        out_specs=HBM,
        scratch_shapes=[pltpu.VMEM(own.shape, F32), pltpu.SemaphoreType.DMA((len(spans(own.shape[1])),))],
        compiler_params=params(16),
        cost_estimate=cost(own.size * len(pieces), 4 * own.size * len(pieces)),
        name="final",
    )(own, *pieces)


def body(blk, pix, particles, ctf, noise_var, projections, orient_class, class_prior, counts):
    rows = projections.shape[0]
    even = list(range(2, blk, 2))
    lead = even[:1] + [0] + even[1:]
    order = lead + [k ^ 1 for k in lead]
    noise, orient_class, class_prior = (value.reshape(1, -1) for value in (noise_var, orient_class, class_prior))
    far = {0: projections}
    near = {}
    for k in even:
        far[k] = swap(projections, "blk", blk, k)
    near[0] = swap(projections, "blk", blk, 1)
    weighted, quadratic, prior = prepare(order, rows, pix, particles, ctf, noise, orient_class, class_prior)
    for k in even:
        near[k] = swap(far[k], "blk", blk, 1)
    lines, square = squares([far[k] for k in lead])
    *chunks, lines, square = score(pix, [near[k] for k in lead], lines, square, weighted, quadratic)
    pieces = []
    for j in range(2, pix):
        pieces.append(swap(chunks[j - 2], "pix", pix, j))
    beside = own_score(pix, 1, lines, square, weighted, quadratic)
    pieces.append(swap(beside, "pix", pix, 1))
    pieces.insert(0, own_score(pix, 0, lines, square, weighted, quadratic))
    weights = weigh(pieces, prior, counts)
    parts = [weights]
    for j in range(1, pix):
        parts.append(swap(weights, "pix", pix, j))
    first = rows
    kept, sent, late, norm = field(parts, weighted, first)
    sent = swap(sent, "blk", blk, 1)
    late = swap(late, "blk", blk, 1)
    out = list(pair(kept, sent, rows, 0, [BF16]))
    own, *last = pair(kept, late, rows, first, [F32] + [BF16] * (len(lead) - 2))
    got = []
    for piece, k in zip(out + last, even):
        got.append(swap(piece, "blk", blk, k))
    return final(own, got), norm.reshape(-1)


def solution(mesh):
    placed = (P("blk", "pix"), P("blk", "pix"), P("pix"), P("blk", "pix"), P(), P(), P("blk"))
    return jax.shard_map(
        functools.partial(body, mesh.shape["blk"], mesh.shape["pix"]),
        mesh=mesh,
        in_specs=placed,
        out_specs=(P("blk", "pix"), P("blk")),
        check_vma=False,
    )
```
